8 devices in a mesh: tube: 2 (over z, y), col: 2 (over x), row: 2 (over core).
Axes of the slice: x: 2, y: 2, z: 1, core: 2. Of those that a mesh axis runs over, the one named last changes fastest.
Arguments:
- tensor: float32 [32, 512, 2048], P('tube', 'row', 'col')
- b_init: float32 [2048, 64], P(('col', 'row', 'tube'))
- c_init: float32 [32, 64], replicated
- ridge_lam: float32 [], replicated
Outputs:
- output 1: float32 [512, 64], P(('row', 'col', 'tube'))
- output 2: float32 [2048, 64], P(('col', 'row', 'tube'))
- output 3: float32 [32, 64], replicated
All inputs are finite; a program needn't handle non-finite values.
Results may differ from the reference program's by a relative error of at most 0.001.
Values are sent between devices in bfloat16 or wider.
A program may use at most 1 GiB of HBM per device.

```python
import jax
import jax.numpy as jnp
from jax import lax

K_LEN = 32
CP_RANK = 64
I_ROWS = 512
J_ROWS = 2048
SWEEPS = 2


def setup_inputs(seed: int = 0) -> dict:
    keys = jax.random.split(jax.random.key(seed), 7)
    scale = CP_RANK ** (-1.0 / 6.0)
    fac_a = scale * jax.random.normal(keys[0], (I_ROWS, CP_RANK), jnp.float32)
    fac_b = scale * jax.random.normal(keys[1], (J_ROWS, CP_RANK), jnp.float32)
    fac_c = scale * jax.random.normal(keys[2], (K_LEN, CP_RANK), jnp.float32)
    kir_prod = fac_c[:, None, :] * fac_a[None, :, :]
    planted = jnp.einsum("kir,jr->kij", kir_prod, fac_b)
    noise = 0.3 * jax.random.normal(keys[3], (K_LEN, I_ROWS, J_ROWS), jnp.float32)
    b_init = fac_b + scale * jax.random.normal(keys[4], (J_ROWS, CP_RANK), jnp.float32)
    c_init = fac_c + scale * jax.random.normal(keys[5], (K_LEN, CP_RANK), jnp.float32)
    ridge_lam = jax.random.uniform(keys[6], (), jnp.float32, 0.1, 0.3) * (J_ROWS * K_LEN * CP_RANK ** (-2.0 / 3.0))
    return {"tensor": planted + noise, "b_init": b_init, "c_init": c_init, "ridge_lam": ridge_lam}


def gram_of(factor):
    half_fac = factor.astype(jnp.bfloat16)
    return jnp.dot(half_fac.T, half_fac, preferred_element_type=jnp.float32)


def solve_rows(mttkrp_rows, gram_prod, ridge_lam):
    ident_mat = jnp.eye(gram_prod.shape[0], dtype=gram_prod.dtype)
    chol_fac = jnp.linalg.cholesky(gram_prod + ridge_lam * ident_mat)
    half_solve = lax.linalg.triangular_solve(chol_fac, mttkrp_rows, left_side=False, lower=True, transpose_a=True)
    return lax.linalg.triangular_solve(chol_fac, half_solve, left_side=False, lower=True)


def reference(tensor, b_init, c_init, ridge_lam):
    x_half = tensor.astype(jnp.bfloat16)
    flat_x = x_half.reshape(K_LEN * I_ROWS, J_ROWS)
    fac_b = b_init
    fac_c = c_init
    gram_b = gram_of(fac_b)
    for sweep_idx in range(SWEEPS):
        gram_c = gram_of(fac_c)
        u_kir = jnp.dot(flat_x, fac_b.astype(jnp.bfloat16), preferred_element_type=jnp.float32).reshape(K_LEN, I_ROWS, CP_RANK)
        mtt_a = jnp.einsum("kir,kr->ir", u_kir.astype(jnp.float32), fac_c.astype(jnp.float32))
        fac_a = solve_rows(mtt_a, gram_b * gram_c, ridge_lam)
        gram_a = gram_of(fac_a)
        a_half = fac_a.astype(jnp.bfloat16)
        v_kjr = lax.map(lambda slab: lax.dot_general(slab, a_half, (((0,), (0,)), ((), ())), preferred_element_type=jnp.float32), x_half)
        mtt_b = jnp.einsum("kjr,kr->jr", v_kjr.astype(jnp.float32), fac_c.astype(jnp.float32))
        fac_b = solve_rows(mtt_b, gram_a * gram_c, ridge_lam)
        gram_b = gram_of(fac_b)
        u_kir = jnp.dot(flat_x, fac_b.astype(jnp.bfloat16), preferred_element_type=jnp.float32).reshape(K_LEN, I_ROWS, CP_RANK)
        mtt_c = jnp.einsum("kir,ir->kr", u_kir.astype(jnp.float32), fac_a.astype(jnp.float32))
        fac_c = solve_rows(mtt_c, gram_a * gram_b, ridge_lam)
    return fac_a, fac_b, fac_c
```

```python
import functools

import jax
import jax.numpy as jnp
from jax import lax
from jax.experimental import pallas as pl
from jax.experimental.pallas import tpu as pltpu
from jax.sharding import PartitionSpec as P

SWEEPS = 2
RANK = 64
LANES = 128
K_LOC = 16
I_LOC = 256
J_TILE = 256
J_TILES = 4
I_HALF = I_LOC // 2
A_CHUNKS = 4
A_CHUNK = I_HALF // A_CHUNKS
BLK = 16
MESH = pl.DeviceIdType.MESH
HIGH = lax.Precision.HIGHEST
F32 = jnp.float32
BF16 = jnp.bfloat16


def dot_nn(a, b, precision=None):
    return lax.dot_general(a, b, (((1,), (0,)), ((), ())), precision=precision, preferred_element_type=F32)


def dot_nt(a, b, precision=None):
    return lax.dot_general(a, b, (((1,), (1,)), ((), ())), precision=precision, preferred_element_type=F32)


def dot_tn(a, b, precision=None):
    return lax.dot_general(a, b, (((0,), (0,)), ((), ())), precision=precision, preferred_element_type=F32)


def inverse_quad(gram_dup, lam):
    row_ids = lax.broadcasted_iota(jnp.int32, (RANK, LANES), 0)
    lane_ids = lax.broadcasted_iota(jnp.int32, (RANK, LANES), 1)
    left_eye = jnp.where(lane_ids == row_ids, 1.0, 0.0).astype(F32)
    right_eye = jnp.where(lane_ids == row_ids + RANK, 1.0, 0.0).astype(F32)
    aug = jnp.where(lane_ids < RANK, gram_dup + lam * left_eye, right_eye)
    n_blk = RANK // BLK
    blocks = [aug[b * BLK:(b + 1) * BLK] for b in range(n_blk)]
    sub_ids = lax.broadcasted_iota(jnp.int32, (BLK, LANES), 0)
    done = []
    for b in range(n_blk):
        piv = blocks[b]
        cols = [jnp.broadcast_to(piv[:, b * BLK + c:b * BLK + c + 1], (BLK, LANES)) for c in range(BLK)]
        mults = [[jnp.broadcast_to(blocks[t][:, b * BLK + c:b * BLK + c + 1], (BLK, LANES)) for c in range(BLK)]
                 for t in range(b + 1, n_blk)]
        chol_rows = jnp.zeros((BLK, LANES), F32)
        for c in range(BLK):
            is_row = sub_ids == c
            root = lax.rsqrt(jnp.broadcast_to(cols[c][c:c + 1, :], (BLK, LANES)))
            scaled_col = cols[c] * root
            scaled_row = jnp.broadcast_to(piv[c:c + 1, :], (BLK, LANES)) * root
            chol_rows = jnp.where(is_row, scaled_row, chol_rows)
            piv = jnp.where(is_row, scaled_row * root, piv - scaled_col * scaled_row)
            for c2 in range(c + 1, BLK):
                scaled_elt = jnp.broadcast_to(cols[c2][c:c + 1, :], (BLK, LANES)) * root
                cols[c2] = jnp.where(is_row, scaled_elt * root, cols[c2] - scaled_col * scaled_elt)
        done.append(chol_rows)
        for t in range(b + 1, n_blk):
            upd = blocks[t]
            for c in range(BLK):
                upd = upd - mults[t - b - 1][c] * jnp.broadcast_to(piv[c:c + 1, :], (BLK, LANES))
            blocks[t] = upd
    chol = jnp.concatenate(done, axis=0)
    inv_dup = jnp.where(lane_ids < RANK, pltpu.roll(chol, RANK, 1), chol)
    return dot_tn(inv_dup, inv_dup, HIGH)


def kernel(x_hbm, b_init, c_init, lam_ref, a_out, b_out, c_out,
           xf, x4, u_ref, bd, bpk, brcv, cd, cb, a_ref, at_ref,
           ma_snd, ma_rcv, ga_snd, ga_rcv, mb_snd, mb_d2d, mb_sum, mb_rcv, bo_ref,
           gb_snd, gb_rcv, gb_all, mc_snd, mc_rcv, mc_all,
           x_sem, b_ss, b_rs, ma_ss, ma_rs, ga_ss, ga_rs, md_ss, md_rs, my_ss, my_rs,
           ag_ss, ag_rs, gb_ss, gb_rs, mc_ss, mc_rs):
    tube, col, row = lax.axis_index("tube"), lax.axis_index("col"), lax.axis_index("row")

    def peer(d):
        t = 1 - tube if d & 4 else tube
        c = 1 - col if d & 2 else col
        r = 1 - row if d & 1 else row
        return (t, c, r)

    def send(src, dst, ss, rs, d):
        return pltpu.make_async_remote_copy(src_ref=src, dst_ref=dst, send_sem=ss, recv_sem=rs,
                                            device_id=peer(d), device_id_type=MESH)

    def load(k):
        return pltpu.make_async_copy(x_hbm.at[k], xf.at[k], x_sem.at[k])

    @pl.loop(0, K_LOC)
    def _(k):
        load(k).start()

    barrier = pltpu.get_barrier_semaphore()
    for d in range(1, 8):
        pl.semaphore_signal(barrier, inc=1, device_id=peer(d), device_id_type=MESH)

    lam = lam_ref[0, 0]
    lanes_b = lax.broadcasted_iota(jnp.int32, (I_HALF, LANES), 1)
    low_half = lanes_b < RANK
    b_own = b_init[...]
    b_lo, b_hi = b_own[:I_HALF], b_own[I_HALF:]
    bpk[...] = jnp.concatenate([b_lo, b_hi], axis=1).astype(BF16)
    cd[...] = jnp.concatenate([c_init[...], c_init[...]], axis=1)
    pl.semaphore_wait(barrier, 7)

    gather = [(5, 0), (4, 1), (1, 2)]
    copies = [send(bpk, brcv.at[n], b_ss.at[n], b_rs.at[n], d) for d, n in gather]
    for cp in copies:
        cp.start()

    def unpack_b(packed, tile):
        wide = packed.astype(F32)
        turned = pltpu.roll(wide, RANK, 1)
        bd[0, tile, 0:I_HALF, :] = jnp.where(low_half, wide, turned).astype(BF16)
        bd[0, tile, I_HALF:, :] = jnp.where(low_half, turned, wide).astype(BF16)

    unpack_b(bpk[...], row * 2 + tube)
    for (d, n), cp in zip(gather, copies):
        cp.wait()
        t2 = 1 - tube if d & 4 else tube
        r2 = 1 - row if d & 1 else row
        unpack_b(brcv[n], r2 * 2 + t2)

    def gram_b_start(slot):
        gram = jnp.zeros((LANES, LANES), F32)
        for jt in range(J_TILES):
            tile = bd[slot, jt]
            gram = gram + dot_tn(tile, tile)
        gb_snd[slot] = gram[:RANK]
        cp = send(gb_snd.at[slot], gb_rcv.at[slot], gb_ss.at[slot], gb_rs.at[slot], 2)
        cp.start()

    def gram_b_finish(slot):
        send(gb_snd.at[slot], gb_rcv.at[slot], gb_ss.at[slot], gb_rs.at[slot], 2).wait()
        gb_all[...] = gb_snd[slot] + gb_rcv[slot]

    def pack_u(u_both):
        return jnp.where(low_half, u_both[:I_HALF], u_both[I_HALF:])

    gram_b_start(0)

    @pl.loop(0, K_LOC)
    def _(k):
        load(k).wait()
        u_both = jnp.zeros((I_LOC, LANES), F32)
        for jt in range(J_TILES):
            xb = xf[k, :, jt * J_TILE:(jt + 1) * J_TILE].astype(BF16)
            x4[jt, k] = xb
            u_both = u_both + dot_nn(xb, bd[0, jt])
        u_ref[k] = pack_u(u_both)

    gram_b_finish(0)

    @pl.loop(0, SWEEPS)
    def _(s):
        k_base = pl.multiple_of(tube * K_LOC, K_LOC)
        c_own = cd[pl.ds(k_base, K_LOC), :]
        a_copies = []
        for ch in range(A_CHUNKS):
            rows = pl.ds(ch * A_CHUNK, A_CHUNK)
            part = jnp.zeros((A_CHUNK, LANES), F32)
            for k in range(K_LOC):
                part = part + u_ref[k, ch * A_CHUNK:(ch + 1) * A_CHUNK, :] * c_own[k:k + 1, :]
            ma_snd[ch * A_CHUNK:(ch + 1) * A_CHUNK, :] = part
            for n, d in ((2, 6), (1, 4), (0, 2)):
                cp = send(ma_snd.at[rows], ma_rcv.at[s, n, rows], ma_ss.at[n, ch], ma_rs.at[s, n, ch], d)
                cp.start()
                a_copies.append(cp)
        c_half = cd[...].astype(BF16)
        gram_c = dot_tn(c_half, c_half)[:RANK]
        c_turn = c_own.T
        for k in range(K_LOC):
            cb[k] = jnp.broadcast_to(c_turn[:RANK, k:k + 1], (RANK, LANES))
        inv_a = inverse_quad(gb_all[...] * gram_c, lam)
        quad_r = lax.broadcasted_iota(jnp.int32, (LANES, LANES), 0) < RANK
        quad_c = lax.broadcasted_iota(jnp.int32, (LANES, LANES), 1) < RANK
        inv_diag = jnp.where(quad_r == quad_c, inv_a, 0.0)
        for cp in a_copies:
            cp.wait()
        mtt_a = (ma_snd[...] + ma_rcv[s, 0]) + (ma_rcv[s, 1] + ma_rcv[s, 2])
        a_new = dot_nn(mtt_a, inv_diag, HIGH)
        a_ref[...] = a_new
        a_turn = a_new.T.astype(BF16)
        at_ref[:, :I_HALF] = a_turn[:RANK]
        at_ref[:, I_HALF:] = a_turn[RANK:]
        at = at_ref[...]
        ga_snd[...] = dot_nt(at, jnp.concatenate([at, at], axis=0))
        ga_cp = send(ga_snd, ga_rcv.at[s], ga_ss, ga_rs.at[s], 1)
        ga_cp.start()

        def v_tile(jt):
            acc = jnp.zeros((RANK, J_TILE), F32)
            for k in range(K_LOC):
                v_kt = dot_nn(at_ref[...], x4[jt, k])
                c_col = cb[k]
                acc = acc + v_kt * jnp.concatenate([c_col, c_col], axis=1)
            return acc

        d_copies = []
        for q in range(2):
            mb_snd[q] = v_tile((1 - row) * 2 + q)
            cp = send(mb_snd.at[q], mb_d2d.at[s, q], md_ss.at[q], md_rs.at[s, q], 1)
            cp.start()
            d_copies.append(cp)
        y_copies = []
        for q in range(2):
            own = v_tile(row * 2 + q)
            d_copies[q].wait()
            mb_sum[q] = own + mb_d2d[s, q]
            cp = send(mb_sum.at[q], mb_rcv.at[s, q], my_ss.at[q], my_rs.at[s, q], 4)
            cp.start()
            y_copies.append(cp)
        ga_cp.wait()
        gram_a = ga_snd[...] + ga_rcv[s]
        inv_b = inverse_quad(gram_a * gram_c, lam)
        g_copies = []
        for q in range(2):
            y_copies[q].wait()
            mtt_b = mb_sum[q] + mb_rcv[s, q]
            b_new = dot_tn(mtt_b, inv_b[:RANK], HIGH)
            bo_ref[q] = b_new
            tile = bd.at[s + 1, row * 2 + q]
            tile[...] = b_new.astype(BF16)
            cp = send(tile, tile, ag_ss.at[q], ag_rs.at[s, q], 1)
            cp.start()
            g_copies.append(cp)
        for cp in g_copies:
            cp.wait()

        gram_b_start(s + 1)

        @pl.loop(0, K_LOC)
        def _(k):
            u_both = jnp.zeros((I_LOC, LANES), F32)
            for jt in range(J_TILES):
                u_both = u_both + dot_nn(x4[jt, k], bd[s + 1, jt])
            u_new = pack_u(u_both)
            u_ref[k] = u_new
            mc_snd[pl.ds(k, 1), :] = jnp.sum(u_new * a_ref[...], axis=0, keepdims=True)

        c_copies = []
        for d in (7, 6, 5, 4, 3, 2, 1):
            cp = send(mc_snd, mc_rcv.at[s, d - 1], mc_ss.at[d - 1], mc_rs.at[s, d - 1], d)
            cp.start()
            c_copies.append(cp)
        gram_b_finish(s + 1)
        inv_c = inverse_quad(gram_a * gb_all[...], lam)
        for cp in c_copies:
            cp.wait()
        near = (mc_snd[...] + mc_rcv[s, 0]) + (mc_rcv[s, 1] + mc_rcv[s, 2])
        far = (mc_rcv[s, 3] + mc_rcv[s, 4]) + (mc_rcv[s, 5] + mc_rcv[s, 6])
        mc_all[pl.ds(k_base, K_LOC), :] = near
        mc_all[pl.ds(pl.multiple_of((1 - tube) * K_LOC, K_LOC), K_LOC), :] = far
        cd[...] = dot_nn(mc_all[...], inv_c, HIGH)

    a_rows = a_ref[pl.ds(pl.multiple_of(tube * RANK, RANK), RANK), :]
    a_out[...] = jnp.where(col == 0, a_rows[:, :RANK], a_rows[:, RANK:])
    b_out[...] = bo_ref[tube][:, :RANK]
    c_out[...] = cd[:, :RANK]


def solution(mesh):
    def local(x_blk, b_own, c_full, ridge_lam):
        dma = pltpu.SemaphoreType.DMA
        vm = pltpu.VMEM
        return pl.pallas_call(
            kernel,
            out_shape=(jax.ShapeDtypeStruct((64, RANK), F32), jax.ShapeDtypeStruct((256, RANK), F32),
                       jax.ShapeDtypeStruct((32, RANK), F32)),
            in_specs=[pl.BlockSpec(memory_space=pl.ANY), pl.BlockSpec(memory_space=pltpu.VMEM),
                      pl.BlockSpec(memory_space=pltpu.VMEM), pl.BlockSpec(memory_space=pltpu.SMEM)],
            out_specs=(pl.BlockSpec(memory_space=pltpu.VMEM),) * 3,
            scratch_shapes=[
                vm((K_LOC, I_LOC, J_TILE * J_TILES), F32),
                vm((J_TILES, K_LOC, I_LOC, J_TILE), BF16),
                vm((K_LOC, I_HALF, LANES), F32),
                vm((SWEEPS + 1, J_TILES, J_TILE, LANES), BF16),
                vm((I_HALF, LANES), BF16),
                vm((3, I_HALF, LANES), BF16),
                vm((2 * K_LOC, LANES), F32),
                vm((K_LOC, RANK, LANES), F32),
                vm((I_HALF, LANES), F32),
                vm((RANK, I_LOC), BF16),
                vm((I_HALF, LANES), F32),
                vm((SWEEPS, 3, I_HALF, LANES), F32),
                vm((RANK, LANES), F32),
                vm((SWEEPS, RANK, LANES), F32),
                vm((2, RANK, J_TILE), F32),
                vm((SWEEPS, 2, RANK, J_TILE), F32),
                vm((2, RANK, J_TILE), F32),
                vm((SWEEPS, 2, RANK, J_TILE), F32),
                vm((2, J_TILE, LANES), F32),
                vm((SWEEPS + 1, RANK, LANES), F32),
                vm((SWEEPS + 1, RANK, LANES), F32),
                vm((RANK, LANES), F32),
                vm((K_LOC, LANES), F32),
                vm((SWEEPS, 7, K_LOC, LANES), F32),
                vm((2 * K_LOC, LANES), F32),
                dma((K_LOC,)), dma((3,)), dma((3,)),
                dma((3, A_CHUNKS)), dma((SWEEPS, 3, A_CHUNKS)),
                dma, dma((SWEEPS,)),
                dma((2,)), dma((SWEEPS, 2)), dma((2,)), dma((SWEEPS, 2)),
                dma((2,)), dma((SWEEPS, 2)),
                dma((SWEEPS + 1,)), dma((SWEEPS + 1,)),
                dma((7,)), dma((SWEEPS, 7)),
            ],
            compiler_params=pltpu.CompilerParams(collective_id=0, has_side_effects=True,
                                                 vmem_limit_bytes=60 * 1024 * 1024),
            name="als_sweeps",
        )(x_blk, b_own, c_full, ridge_lam.reshape(1, 1))

    return jax.shard_map(
        local,
        mesh=mesh,
        in_specs=(P("tube", "row", "col"), P(("col", "row", "tube"), None), P(None, None), P()),
        out_specs=(P(("row", "col", "tube"), None), P(("col", "row", "tube"), None), P(None, None)),
        check_vma=False,
    )
```

```python
import functools

import jax
import jax.numpy as jnp
from jax import lax
from jax.experimental import pallas as pl
from jax.experimental.pallas import tpu as pltpu
from jax.sharding import PartitionSpec as P

SWEEPS = 2
RANK = 64
LANES = 128
K_LOC = 16
I_LOC = 256
J_TILE = 256
J_TILES = 4
I_HALF = I_LOC // 2
A_CHUNKS = 4
A_CHUNK = I_HALF // A_CHUNKS
BLK = 16
LOAD_K = 4
MESH = pl.DeviceIdType.MESH
HIGH = lax.Precision.HIGHEST
F32 = jnp.float32
BF16 = jnp.bfloat16


def dot_nn(a, b, precision=None):
    return lax.dot_general(a, b, (((1,), (0,)), ((), ())), precision=precision, preferred_element_type=F32)


def dot_nt(a, b, precision=None):
    return lax.dot_general(a, b, (((1,), (1,)), ((), ())), precision=precision, preferred_element_type=F32)


def dot_tn(a, b, precision=None):
    return lax.dot_general(a, b, (((0,), (0,)), ((), ())), precision=precision, preferred_element_type=F32)


def inverse_quad(gram_dup, lam):
    row_ids = lax.broadcasted_iota(jnp.int32, (RANK, LANES), 0)
    lane_ids = lax.broadcasted_iota(jnp.int32, (RANK, LANES), 1)
    left_eye = jnp.where(lane_ids == row_ids, 1.0, 0.0).astype(F32)
    right_eye = jnp.where(lane_ids == row_ids + RANK, 1.0, 0.0).astype(F32)
    aug = jnp.where(lane_ids < RANK, gram_dup + lam * left_eye, right_eye)
    n_blk = RANK // BLK
    blocks = [aug[b * BLK:(b + 1) * BLK] for b in range(n_blk)]
    sub_ids = lax.broadcasted_iota(jnp.int32, (BLK, LANES), 0)
    done = []
    for b in range(n_blk):
        piv = blocks[b]
        cols = [jnp.broadcast_to(piv[:, b * BLK + c:b * BLK + c + 1], (BLK, LANES)) for c in range(BLK)]
        mults = [[jnp.broadcast_to(blocks[t][:, b * BLK + c:b * BLK + c + 1], (BLK, LANES)) for c in range(BLK)]
                 for t in range(b + 1, n_blk)]
        chol_rows = jnp.zeros((BLK, LANES), F32)
        for c in range(BLK):
            is_row = sub_ids == c
            root = lax.rsqrt(jnp.broadcast_to(cols[c][c:c + 1, :], (BLK, LANES)))
            scaled_col = cols[c] * root
            scaled_row = jnp.broadcast_to(piv[c:c + 1, :], (BLK, LANES)) * root
            chol_rows = jnp.where(is_row, scaled_row, chol_rows)
            piv = jnp.where(is_row, scaled_row * root, piv - scaled_col * scaled_row)
            for c2 in range(c + 1, BLK):
                scaled_elt = jnp.broadcast_to(cols[c2][c:c + 1, :], (BLK, LANES)) * root
                cols[c2] = jnp.where(is_row, scaled_elt * root, cols[c2] - scaled_col * scaled_elt)
        done.append(chol_rows)
        for t in range(b + 1, n_blk):
            upd = blocks[t]
            for c in range(BLK):
                upd = upd - mults[t - b - 1][c] * jnp.broadcast_to(piv[c:c + 1, :], (BLK, LANES))
            blocks[t] = upd
    chol = jnp.concatenate(done, axis=0)
    inv_dup = jnp.where(lane_ids < RANK, pltpu.roll(chol, RANK, 1), chol)
    return dot_tn(inv_dup, inv_dup, HIGH)


def kernel(x_hbm, b_hbm, c_hbm, lam_ref, a_out, b_out, c_out,
           b_init, c_init, xf, x4, u_ref, bd, bpk, brcv, cd, cb, a_ref, at_ref,
           ma_snd, ma_rcv, ga_snd, ga_rcv, mb_snd, mb_d2d, mb_sum, mb_rcv, bo_ref,
           g0_snd, g0_rcv, gb_snd, gb_rcv, gb_all, mc_full, mc_snd, mc_rcv, inv_ref,
           in_sem, x_sem, b_ss, b_rs, ma_ss, ma_rs, ga_ss, ga_rs, md_ss, md_rs, my_ss, my_rs,
           ag_ss, ag_rs, g0_ss, g0_rs, gb_ss, gb_rs, mc_ss, mc_rs):
    tube, col, row = lax.axis_index("tube"), lax.axis_index("col"), lax.axis_index("row")

    def peer(d):
        t = 1 - tube if d & 4 else tube
        c = 1 - col if d & 2 else col
        r = 1 - row if d & 1 else row
        return (t, c, r)

    def send(src, dst, ss, rs, d):
        return pltpu.make_async_remote_copy(src_ref=src, dst_ref=dst, send_sem=ss, recv_sem=rs,
                                            device_id=peer(d), device_id_type=MESH)

    def load(n, g):
        rows = pl.ds(g * LOAD_K, LOAD_K)
        return pltpu.make_async_copy(x_hbm.at[rows, :, pl.ds(pl.multiple_of(tile_of(n) * J_TILE, J_TILE), J_TILE)],
                                     xf.at[n, rows], x_sem.at[n, g])

    def tile_of(n):
        r = 1 - row if n & 1 else row
        t = 1 - tube if n & 2 else tube
        return r * 2 + t

    small = [pltpu.make_async_copy(b_hbm, b_init, in_sem.at[0]), pltpu.make_async_copy(c_hbm, c_init, in_sem.at[1])]
    for cp in small:
        cp.start()

    def load_start(n):
        for g in range(K_LOC // LOAD_K):
            load(n, g).start()

    load_start(0)
    barrier = pltpu.get_barrier_semaphore()
    for d in range(1, 8):
        pl.semaphore_signal(barrier, inc=1, device_id=peer(d), device_id_type=MESH)

    lam = lam_ref[0, 0]
    lanes_b = lax.broadcasted_iota(jnp.int32, (I_HALF, LANES), 1)
    low_half = lanes_b < RANK
    for cp in small:
        cp.wait()
    for n in range(1, J_TILES):
        load_start(n)
    b_turn = b_init[...]
    bpk[...] = jnp.concatenate([b_turn[:, :I_HALF], b_turn[:, I_HALF:]], axis=0).T.astype(BF16)
    cd[...] = jnp.concatenate([c_init[...], c_init[...]], axis=1)
    pl.semaphore_wait(barrier, 7)

    def b_send(n):
        return send(bpk, brcv.at[n - 1], b_ss.at[n - 1], b_rs.at[n - 1], (n & 1) | (n & 2) << 1)

    for n in (3, 2, 1):
        b_send(n).start()

    def unpack_b(packed, n):
        wide = packed.astype(F32)
        turned = pltpu.roll(wide, RANK, 1)
        tile = tile_of(n)
        bd[0, tile, 0:I_HALF, :] = jnp.where(low_half, wide, turned).astype(BF16)
        bd[0, tile, I_HALF:, :] = jnp.where(low_half, turned, wide).astype(BF16)

    half_lanes = lax.broadcasted_iota(jnp.int32, (RANK // 2, LANES), 1) < RANK

    def gram_pack(tiles):
        gram = sum(dot_tn(tile, tile)[:RANK] for tile in tiles)
        return jnp.where(half_lanes, gram[:RANK // 2], gram[RANK // 2:])

    def gram_unpack(packed):
        turned = pltpu.roll(packed, RANK, 1)
        return jnp.concatenate([jnp.where(half_lanes, packed, turned), jnp.where(half_lanes, turned, packed)], axis=0)

    def g0_send(d):
        return send(g0_snd, g0_rcv.at[d - 1], g0_ss.at[d - 1], g0_rs.at[d - 1], d)

    def gb_send(s, d):
        return send(gb_snd, gb_rcv.at[s, d - 1], gb_ss.at[d - 1], gb_rs.at[s, d - 1], d)

    def gram_b_start(s):
        gb_snd[...] = gram_pack([bd[s + 1, row * 2], bd[s + 1, row * 2 + 1]])
        for d in (3, 2, 1):
            gb_send(s, d).start()

    def gram_b_finish(s):
        for d in (3, 2, 1):
            gb_send(s, d).wait()
        gb_all[...] = gram_unpack((gb_snd[...] + gb_rcv[s, 0]) + (gb_rcv[s, 1] + gb_rcv[s, 2]))

    def pack_u(u_both):
        return jnp.where(low_half, u_both[:I_HALF], u_both[I_HALF:])

    def u_pass(slot, tiles, first, last, staged=None):
        for k in range(K_LOC):
            u_both = jnp.zeros((I_LOC, LANES), F32)
            for jt in tiles:
                if staged is None:
                    x_tile = x4[jt, k]
                else:
                    x_tile = xf[staged, k].astype(BF16)
                    x4[jt, k] = x_tile
                u_both = u_both + dot_nn(x_tile, bd[slot, jt])
            u_new = pack_u(u_both)
            if not first:
                u_new = u_ref[k] + u_new
            u_ref[k] = u_new
            if last:
                mc_full[k:k + 1, :] = jnp.sum(u_new * a_ref[...], axis=0, keepdims=True)

    unpack_b(bpk[...], 0)
    g0_snd[...] = gram_pack([bd[0, tile_of(0)]])
    for d in (7, 6, 3, 2, 5, 4, 1):
        g0_send(d).start()
    for n in range(J_TILES):
        if n > 0:
            b_send(n).wait()
            unpack_b(brcv[n - 1], n)
        for g in range(K_LOC // LOAD_K):
            load(n, g).wait()
        u_pass(0, [tile_of(n)], n == 0, False, staged=n)
    for d in range(1, 8):
        g0_send(d).wait()
    here = (g0_snd[...] + g0_rcv[0]) + (g0_rcv[3] + g0_rcv[4])
    there = (g0_rcv[1] + g0_rcv[2]) + (g0_rcv[5] + g0_rcv[6])
    gb_all[...] = gram_unpack(here + there)

    k_base = pl.multiple_of(tube * K_LOC, K_LOC)
    k_far = pl.multiple_of((1 - tube) * K_LOC, K_LOC)

    def c_send(s, d):
        return send(mc_snd, mc_rcv.at[s, d - 1], mc_ss.at[d - 1], mc_rs.at[s, d - 1], d)

    def c_solve(packed):
        low = lax.broadcasted_iota(jnp.int32, packed.shape, 1) < RANK
        split = jnp.concatenate([jnp.where(low, packed, 0.0), jnp.where(low, 0.0, packed)], axis=0)
        return dot_nn(split, inv_ref[...], HIGH)

    def c_far(s):
        for d in (4, 5, 6, 7):
            c_send(s, d).wait()
        far = (mc_rcv[s, 3] + mc_rcv[s, 4]) + (mc_rcv[s, 5] + mc_rcv[s, 6])
        cd[pl.ds(k_far, K_LOC), :] = c_solve(far)

    @pl.loop(0, SWEEPS)
    def _(s):
        c_own = cd[pl.ds(k_base, K_LOC), :]
        a_copies = []
        for ch in range(A_CHUNKS):
            rows = pl.ds(ch * A_CHUNK, A_CHUNK)
            part = jnp.zeros((A_CHUNK, LANES), F32)
            for k in range(K_LOC):
                part = part + u_ref[k, ch * A_CHUNK:(ch + 1) * A_CHUNK, :] * c_own[k:k + 1, :]
            ma_snd[ch * A_CHUNK:(ch + 1) * A_CHUNK, :] = part
            for n, d in ((2, 6), (1, 4), (0, 2)):
                cp = send(ma_snd.at[rows], ma_rcv.at[s, n, rows], ma_ss.at[n, ch], ma_rs.at[s, n, ch], d)
                cp.start()
                a_copies.append(cp)
        @pl.when(s > 0)
        def _():
            c_far(s - 1)

        c_half = cd[...].astype(BF16)
        gram_c = dot_tn(c_half, c_half)[:RANK]
        c_turn = c_own.T
        for k in range(K_LOC):
            cb[k] = jnp.broadcast_to(c_turn[:RANK, k:k + 1], (RANK, LANES))
        inv_a = inverse_quad(gb_all[...] * gram_c, lam)
        quad_r = lax.broadcasted_iota(jnp.int32, (LANES, LANES), 0) < RANK
        quad_c = lax.broadcasted_iota(jnp.int32, (LANES, LANES), 1) < RANK
        inv_diag = jnp.where(quad_r == quad_c, inv_a, 0.0)
        for cp in a_copies:
            cp.wait()
        mtt_a = (ma_snd[...] + ma_rcv[s, 0]) + (ma_rcv[s, 1] + ma_rcv[s, 2])
        a_new = dot_nn(mtt_a, inv_diag, HIGH)
        a_ref[...] = a_new
        a_turn = a_new.T.astype(BF16)
        at_ref[:, :I_HALF] = a_turn[:RANK]
        at_ref[:, I_HALF:] = a_turn[RANK:]

        def v_tile(jt):
            acc = jnp.zeros((RANK, J_TILE), F32)
            for k in range(K_LOC):
                v_kt = dot_nn(at_ref[...], x4[jt, k])
                c_col = cb[k]
                acc = acc + v_kt * jnp.concatenate([c_col, c_col], axis=1)
            return acc

        d_copies = []
        for q in range(2):
            mb_snd[q] = v_tile((1 - row) * 2 + q)
            cp = send(mb_snd.at[q], mb_d2d.at[s, q], md_ss.at[q], md_rs.at[s, q], 1)
            cp.start()
            d_copies.append(cp)
            if q == 0:
                at = at_ref[...]
                ga_snd[...] = dot_nt(at, jnp.concatenate([at, at], axis=0))
                ga_cp = send(ga_snd, ga_rcv.at[s], ga_ss, ga_rs.at[s], 1)
                ga_cp.start()
        y_copies = []
        for q in range(2):
            own = v_tile(row * 2 + q)
            d_copies[q].wait()
            mb_sum[q] = own + mb_d2d[s, q]
            cp = send(mb_sum.at[q], mb_rcv.at[s, q], my_ss.at[q], my_rs.at[s, q], 4)
            cp.start()
            y_copies.append(cp)
        ga_cp.wait()
        gram_a = ga_snd[...] + ga_rcv[s]
        inv_b = inverse_quad(gram_a * gram_c, lam)
        g_copies = []

        def b_solve(q):
            y_copies[q].wait()
            b_new = dot_tn(mb_sum[q] + mb_rcv[s, q], inv_b[:RANK], HIGH)
            bo_ref[q] = b_new
            tile = bd.at[s + 1, row * 2 + q]
            tile[...] = b_new.astype(BF16)
            cp = send(tile, tile, ag_ss.at[q], ag_rs.at[s, q], 1)
            cp.start()
            g_copies.append(cp)

        b_solve(0)
        u_pass(s + 1, [row * 2], True, False)
        b_solve(1)
        gram_b_start(s)
        g_copies[0].wait()
        u_pass(s + 1, [row * 2 + 1, (1 - row) * 2], False, False)
        g_copies[1].wait()
        u_pass(s + 1, [(1 - row) * 2 + 1], False, True)

        part_c = mc_full[...]
        part_c = part_c + pltpu.roll(part_c, RANK, 1)
        low_c = lax.broadcasted_iota(jnp.int32, (K_LOC // 2, LANES), 1) < RANK
        mc_snd[...] = jnp.where(low_c, part_c[:K_LOC // 2], part_c[K_LOC // 2:])
        for d in (2, 3, 1, 6, 7, 4, 5):
            c_send(s, d).start()
        gram_b_finish(s)
        inv_ref[...] = inverse_quad(gram_a * gb_all[...], lam)
        for d in (1, 2, 3):
            c_send(s, d).wait()
        near = (mc_snd[...] + mc_rcv[s, 0]) + (mc_rcv[s, 1] + mc_rcv[s, 2])
        cd[pl.ds(k_base, K_LOC), :] = c_solve(near)

    c_far(SWEEPS - 1)
    a_rows = a_ref[pl.ds(pl.multiple_of(tube * RANK, RANK), RANK), :]
    a_out[...] = jnp.where(col == 0, a_rows[:, :RANK], a_rows[:, RANK:])
    b_out[...] = bo_ref[tube].T[:RANK]
    c_out[...] = cd[:, :RANK]


def emit(a_in, b_in, c_in, a_hbm, b_hbm, c_hbm, sems):
    pairs = ((b_in, b_hbm), (a_in, a_hbm), (c_in, c_hbm))
    copies = [pltpu.make_async_copy(src, dst, sems.at[n]) for n, (src, dst) in enumerate(pairs)]
    for cp in copies:
        cp.start()
    for cp in copies:
        cp.wait()


def solution(mesh):
    def local(x_blk, b_own, c_full, ridge_lam):
        shapes = ((64, RANK), (RANK, 256), (32, RANK))
        x_blk, b_turn, c_full = (pltpu.with_memory_space_constraint(v, pltpu.HBM) for v in (x_blk, b_own.T, c_full))
        dma = pltpu.SemaphoreType.DMA
        vm = pltpu.VMEM
        a_new, b_new, c_new = pl.pallas_call(
            kernel,
            out_shape=tuple(pltpu.VMEM(shape, F32) for shape in shapes),
            in_specs=[pl.BlockSpec(memory_space=pltpu.HBM), pl.BlockSpec(memory_space=pltpu.HBM),
                      pl.BlockSpec(memory_space=pltpu.HBM), pl.BlockSpec(memory_space=pltpu.SMEM)],
            out_specs=(pl.BlockSpec(memory_space=pltpu.VMEM),) * 3,
            scratch_shapes=[
                vm((RANK, 256), F32),
                vm((2 * K_LOC, RANK), F32),
                vm((J_TILES, K_LOC, I_LOC, J_TILE), F32),
                vm((J_TILES, K_LOC, I_LOC, J_TILE), BF16),
                vm((K_LOC, I_HALF, LANES), F32),
                vm((SWEEPS + 1, J_TILES, J_TILE, LANES), BF16),
                vm((I_HALF, LANES), BF16),
                vm((3, I_HALF, LANES), BF16),
                vm((2 * K_LOC, LANES), F32),
                vm((K_LOC, RANK, LANES), F32),
                vm((I_HALF, LANES), F32),
                vm((RANK, I_LOC), BF16),
                vm((I_HALF, LANES), F32),
                vm((SWEEPS, 3, I_HALF, LANES), F32),
                vm((RANK, LANES), F32),
                vm((SWEEPS, RANK, LANES), F32),
                vm((2, RANK, J_TILE), F32),
                vm((SWEEPS, 2, RANK, J_TILE), F32),
                vm((2, RANK, J_TILE), F32),
                vm((SWEEPS, 2, RANK, J_TILE), F32),
                vm((2, J_TILE, LANES), F32),
                vm((RANK // 2, LANES), F32),
                vm((7, RANK // 2, LANES), F32),
                vm((RANK // 2, LANES), F32),
                vm((SWEEPS, 3, RANK // 2, LANES), F32),
                vm((RANK, LANES), F32),
                vm((K_LOC, LANES), F32),
                vm((K_LOC // 2, LANES), F32),
                vm((SWEEPS, 7, K_LOC // 2, LANES), F32),
                vm((LANES, LANES), F32),
                dma((2,)), dma((J_TILES, K_LOC // LOAD_K)), dma((3,)), dma((3,)),
                dma((3, A_CHUNKS)), dma((SWEEPS, 3, A_CHUNKS)),
                dma, dma((SWEEPS,)),
                dma((2,)), dma((SWEEPS, 2)), dma((2,)), dma((SWEEPS, 2)),
                dma((2,)), dma((SWEEPS, 2)),
                dma((7,)), dma((7,)), dma((3,)), dma((SWEEPS, 3)),
                dma((7,)), dma((SWEEPS, 7)),
            ],
            compiler_params=pltpu.CompilerParams(collective_id=0, has_side_effects=True,
                                                 vmem_limit_bytes=52 * 1024 * 1024),
            name="als_sweeps",
        )(x_blk, b_turn, c_full, ridge_lam.reshape(1, 1))
        a_new, b_new, c_new = pl.pallas_call(
            emit,
            out_shape=tuple(jax.ShapeDtypeStruct(shape, F32) for shape in shapes),
            in_specs=[pl.BlockSpec(memory_space=pltpu.VMEM)] * 3,
            out_specs=(pl.BlockSpec(memory_space=pl.ANY),) * 3,
            scratch_shapes=[dma((3,))],
            compiler_params=pltpu.CompilerParams(vmem_limit_bytes=1024 * 1024),
            name="emit_factors",
        )(a_new, b_new, c_new)
        return a_new, b_new.T, c_new

    return jax.shard_map(
        local,
        mesh=mesh,
        in_specs=(P("tube", "row", "col"), P(("col", "row", "tube"), None), P(None, None), P()),
        out_specs=(P(("row", "col", "tube"), None), P(("col", "row", "tube"), None), P(None, None)),
        check_vma=False,
    )
```

```python
import functools

import jax
import jax.numpy as jnp
from jax import lax
from jax.experimental import pallas as pl
from jax.experimental.pallas import tpu as pltpu
from jax.sharding import PartitionSpec as P

SWEEPS = 2
RANK = 64
LANES = 128
K_LOC = 16
I_LOC = 256
J_TILE = 256
J_TILES = 4
I_HALF = I_LOC // 2
A_CHUNKS = 2
A_CHUNK = I_HALF // A_CHUNKS
BLK = 16
LOAD_K = 4
MESH = pl.DeviceIdType.MESH
HIGH = lax.Precision.HIGHEST
F32 = jnp.float32
BF16 = jnp.bfloat16


def dot_nn(a, b, precision=None):
    return lax.dot_general(a, b, (((1,), (0,)), ((), ())), precision=precision, preferred_element_type=F32)


def dot_nt(a, b, precision=None):
    return lax.dot_general(a, b, (((1,), (1,)), ((), ())), precision=precision, preferred_element_type=F32)


def dot_tn(a, b, precision=None):
    return lax.dot_general(a, b, (((0,), (0,)), ((), ())), precision=precision, preferred_element_type=F32)


def inverse_quad(gram_dup, lam, between=None):
    row_ids = lax.broadcasted_iota(jnp.int32, (RANK, LANES), 0)
    lane_ids = lax.broadcasted_iota(jnp.int32, (RANK, LANES), 1)
    left_eye = jnp.where(lane_ids == row_ids, 1.0, 0.0).astype(F32)
    right_eye = jnp.where(lane_ids == row_ids + RANK, 1.0, 0.0).astype(F32)
    aug = jnp.where(lane_ids < RANK, gram_dup + lam * left_eye, right_eye)
    n_blk = RANK // BLK
    blocks = [aug[b * BLK:(b + 1) * BLK] for b in range(n_blk)]
    sub_ids = lax.broadcasted_iota(jnp.int32, (BLK, LANES), 0)
    done = []
    for b in range(n_blk):
        piv = blocks[b]
        cols = [jnp.broadcast_to(piv[:, b * BLK + c:b * BLK + c + 1], (BLK, LANES)) for c in range(BLK)]
        mults = [[jnp.broadcast_to(blocks[t][:, b * BLK + c:b * BLK + c + 1], (BLK, LANES)) for c in range(BLK)]
                 for t in range(b + 1, n_blk)]
        chol_rows = jnp.zeros((BLK, LANES), F32)
        for c in range(BLK):
            is_row = sub_ids == c
            root = lax.rsqrt(jnp.broadcast_to(cols[c][c:c + 1, :], (BLK, LANES)))
            scaled_col = cols[c] * root
            scaled_row = jnp.broadcast_to(piv[c:c + 1, :], (BLK, LANES)) * root
            chol_rows = jnp.where(is_row, scaled_row, chol_rows)
            piv = jnp.where(is_row, scaled_row * root, piv - scaled_col * scaled_row)
            for c2 in range(c + 1, BLK):
                scaled_elt = jnp.broadcast_to(cols[c2][c:c + 1, :], (BLK, LANES)) * root
                cols[c2] = jnp.where(is_row, scaled_elt * root, cols[c2] - scaled_col * scaled_elt)
        done.append(chol_rows)
        for t in range(b + 1, n_blk):
            upd = blocks[t]
            for c in range(BLK):
                upd = upd - mults[t - b - 1][c] * jnp.broadcast_to(piv[c:c + 1, :], (BLK, LANES))
            blocks[t] = upd
        if between is not None:
            between(b)
    chol = jnp.concatenate(done, axis=0)
    inv_dup = jnp.where(lane_ids < RANK, pltpu.roll(chol, RANK, 1), chol)
    return dot_tn(inv_dup, inv_dup, HIGH)


def kernel(x_hbm, b_hbm, c_hbm, lam_ref, a_out, b_out, c_out,
           b_init, c_init, xf, x4, u_ref, bd, bpk, brcv, cd, cb, a_ref, at_ref,
           ma_snd, ma_rcv, ga_snd, ga_rcv, mb_part, mb_d2d, mb_sum, mb_rcv, bo_ref,
           g0_snd, g0_rcv, gb_snd, gb_rcv, gb_all, mc_full, mc_snd, mc_rcv, inv_ref,
           in_sem, x_sem, b_ss, b_rs, ma_ss, ma_rs, ga_ss, ga_rs, md_ss, md_rs, my_ss, my_rs,
           ag_ss, ag_rs, g0_ss, g0_rs, gb_ss, gb_rs, mc_ss, mc_rs):
    tube, col, row = lax.axis_index("tube"), lax.axis_index("col"), lax.axis_index("row")

    def peer(d):
        t = 1 - tube if d & 4 else tube
        c = 1 - col if d & 2 else col
        r = 1 - row if d & 1 else row
        return (t, c, r)

    def send(src, dst, ss, rs, d):
        return pltpu.make_async_remote_copy(src_ref=src, dst_ref=dst, send_sem=ss, recv_sem=rs,
                                            device_id=peer(d), device_id_type=MESH)

    def load(n, g):
        rows = pl.ds(g * LOAD_K, LOAD_K)
        return pltpu.make_async_copy(x_hbm.at[rows, :, pl.ds(pl.multiple_of(tile_of(n) * J_TILE, J_TILE), J_TILE)],
                                     xf.at[n, rows], x_sem.at[n, g])

    def tile_of(n):
        if n == 0:
            return row * 2 + tube
        if n == 1:
            return (1 - row) * 2 + tube
        return (3 - n) * 2 + 1 - tube

    small = [pltpu.make_async_copy(src, dst, in_sem.at[n])
             for n, (src, dst) in enumerate(((b_hbm, b_init), (c_hbm, c_init)))]
    for cp in small:
        cp.start()

    def load_start(n):
        for g in range(K_LOC // LOAD_K):
            load(n, g).start(priority=1)

    load_start(0)
    load_start(1)
    barrier = pltpu.get_barrier_semaphore()
    for d in range(1, 8):
        pl.semaphore_signal(barrier, inc=1, device_id=peer(d), device_id_type=MESH)

    lanes_b = lax.broadcasted_iota(jnp.int32, (I_HALF, LANES), 1)
    low_half = lanes_b < RANK
    for cp in small:
        cp.wait()
    for n in range(2, J_TILES):
        load_start(n)
    lam = lam_ref[0, 0]
    b_turn = b_init[...]
    bpk[...] = jnp.concatenate([b_turn[:, :I_HALF], b_turn[:, I_HALF:]], axis=0).T.astype(BF16)
    cd[...] = jnp.concatenate([c_init[...], c_init[...]], axis=1)
    pl.semaphore_wait(barrier, 7)

    def b_send(src, n, d, ss):
        return send(src, brcv.at[n - 1], b_ss.at[ss], b_rs.at[n - 1], d)

    @pl.when(row == 0)
    def _():
        b_send(bpk, 3, 4, 1).start()
        b_send(bpk, 3, 5, 2).start()

    @pl.when(row == 1)
    def _():
        b_send(bpk, 2, 4, 1).start()

    b_send(bpk, 1, 1, 0).start()

    def unpack_b(packed, n):
        wide = packed.astype(F32)
        turned = pltpu.roll(wide, RANK, 1)
        tile = tile_of(n)
        bd[0, tile, 0:I_HALF, :] = jnp.where(low_half, wide, turned).astype(BF16)
        bd[0, tile, I_HALF:, :] = jnp.where(low_half, turned, wide).astype(BF16)

    half_lanes = lax.broadcasted_iota(jnp.int32, (RANK // 2, LANES), 1) < RANK

    def gram_pack(tiles):
        gram = sum(dot_tn(tile, tile)[:RANK] for tile in tiles)
        return jnp.where(half_lanes, gram[:RANK // 2], gram[RANK // 2:])

    def gram_unpack(packed):
        turned = pltpu.roll(packed, RANK, 1)
        return jnp.concatenate([jnp.where(half_lanes, packed, turned), jnp.where(half_lanes, turned, packed)], axis=0)

    def g0_send(d):
        return send(g0_snd, g0_rcv.at[d - 1], g0_ss.at[d - 1], g0_rs.at[d - 1], d)

    def gb_send(s, d):
        return send(gb_snd, gb_rcv.at[s, d - 1], gb_ss.at[d - 1], gb_rs.at[s, d - 1], d)

    def gram_b_start(s):
        gb_snd[...] = gram_pack([bd[s + 1, row * 2], bd[s + 1, row * 2 + 1]])
        for d in (2, 3, 1):
            gb_send(s, d).start()

    def gram_b_finish(s):
        for d in (3, 2, 1):
            gb_send(s, d).wait()
        gb_all[...] = gram_unpack((gb_snd[...] + gb_rcv[s, 0]) + (gb_rcv[s, 1] + gb_rcv[s, 2]))

    low_chunk = lax.broadcasted_iota(jnp.int32, (A_CHUNK, LANES), 1) < RANK

    def pack_u(u_both):
        quarters = [u_both[n * A_CHUNK:(n + 1) * A_CHUNK] for n in range(2 * A_CHUNKS)]
        return jnp.concatenate([jnp.where(low_chunk, quarters[2 * c], quarters[2 * c + 1])
                                for c in range(A_CHUNKS)], axis=0)

    def u_pass(slot, tiles, first, last, staged=None, slabs=range(K_LOC)):
        for k in slabs:
            u_both = jnp.zeros((I_LOC, LANES), F32)
            for jt in tiles:
                if staged is None:
                    x_tile = x4[jt, k]
                else:
                    x_tile = xf[staged, k].astype(BF16)
                    x4[jt, k] = x_tile
                u_both = u_both + dot_nn(x_tile, bd[slot, jt])
            u_new = pack_u(u_both)
            if not first:
                u_new = u_ref[k] + u_new
            u_ref[k] = u_new
            if last:
                mc_full[k:k + 1, :] = jnp.sum(u_new * a_ref[...], axis=0, keepdims=True)

    unpack_b(bpk[...], 0)
    g0_snd[...] = gram_pack([bd[0, tile_of(0)]])
    for d in (7, 6, 3, 2, 5, 4, 1):
        g0_send(d).start()
    for n in range(J_TILES):
        if n > 0:
            b_send(bpk, n, 1, 0).wait_recv()
            if n == 2:
                @pl.when(row == 1)
                def _():
                    b_send(brcv.at[1], 2, 1, 2).start()
            unpack_b(brcv[n - 1], n)
        step = K_LOC // 2 if n == J_TILES - 1 else K_LOC
        for k in range(0, K_LOC, step):
            for g in range(k // LOAD_K, (k + step) // LOAD_K):
                load(n, g).wait()
            u_pass(0, [tile_of(n)], n == 0, False, staged=n, slabs=range(k, k + step))
    for ss in range(3):
        b_send(bpk, 1, 1, ss).wait_send()
    for d in range(1, 8):
        g0_send(d).wait()
    here = (g0_snd[...] + g0_rcv[0]) + (g0_rcv[3] + g0_rcv[4])
    there = (g0_rcv[1] + g0_rcv[2]) + (g0_rcv[5] + g0_rcv[6])
    gb_all[...] = gram_unpack(here + there)

    k_base = pl.multiple_of(tube * K_LOC, K_LOC)
    k_far = pl.multiple_of((1 - tube) * K_LOC, K_LOC)

    def c_send(s, d):
        return send(mc_snd, mc_rcv.at[s, d - 1], mc_ss.at[d - 1], mc_rs.at[s, d - 1], d)

    def c_solve(packed):
        low = lax.broadcasted_iota(jnp.int32, packed.shape, 1) < RANK
        split = jnp.concatenate([jnp.where(low, packed, 0.0), jnp.where(low, 0.0, packed)], axis=0)
        return dot_nn(split, inv_ref[...], HIGH)

    def c_far(s):
        for d in (4, 5, 6, 7):
            c_send(s, d).wait()
        far = (mc_rcv[s, 3] + mc_rcv[s, 4]) + (mc_rcv[s, 5] + mc_rcv[s, 6])
        cd[pl.ds(k_far, K_LOC), :] = c_solve(far)

    @pl.loop(0, SWEEPS)
    def _(s):
        c_own = cd[pl.ds(k_base, K_LOC), :]
        def a_send(ch, d):
            rows = pl.ds(ch * A_CHUNK, A_CHUNK)
            n = d // 2 - 1
            return send(ma_snd.at[rows], ma_rcv.at[s, n, rows], ma_ss.at[n, ch], ma_rs.at[s, n, ch], d)

        for ch in range(A_CHUNKS):
            part = jnp.zeros((A_CHUNK, LANES), F32)
            for k in range(K_LOC):
                part = part + u_ref[k, ch * A_CHUNK:(ch + 1) * A_CHUNK, :] * c_own[k:k + 1, :]
            ma_snd[ch * A_CHUNK:(ch + 1) * A_CHUNK, :] = part
            for d in (6, 4, 2):
                a_send(ch, d).start()

        @pl.when(s > 0)
        def _():
            c_far(s - 1)

        c_half = cd[...].astype(BF16)
        gram_c = dot_tn(c_half, c_half)[:RANK]
        c_turn = c_own.T
        for k in range(K_LOC):
            cb[k] = jnp.broadcast_to(c_turn[:RANK, k:k + 1], (RANK, LANES))
        inv_a = inverse_quad(gb_all[...] * gram_c, lam)
        quad_r = lax.broadcasted_iota(jnp.int32, (LANES, LANES), 0) < RANK
        quad_c = lax.broadcasted_iota(jnp.int32, (LANES, LANES), 1) < RANK
        inv_diag = jnp.where(quad_r == quad_c, inv_a, 0.0)

        def a_solve(ch):
            rows = slice(ch * A_CHUNK, (ch + 1) * A_CHUNK)
            for d in (2, 4, 6):
                a_send(ch, d).wait()
            mtt_a = (ma_snd[rows, :] + ma_rcv[s, 0, rows, :]) + (ma_rcv[s, 1, rows, :] + ma_rcv[s, 2, rows, :])
            a_new = dot_nn(mtt_a, inv_diag, HIGH)
            a_ref[rows, :] = a_new
            a_turn = a_new.T
            at_ref[ch] = jnp.concatenate([a_turn[:RANK], a_turn[RANK:]], axis=1).astype(BF16)

        def v_tile(jt, ch):
            acc = jnp.zeros((RANK, J_TILE), F32)
            for k in range(K_LOC):
                v_kt = dot_nn(at_ref[ch], x4[jt, k, ch * I_HALF:(ch + 1) * I_HALF, :])
                c_col = cb[k]
                acc = acc + v_kt * jnp.concatenate([c_col, c_col], axis=1)
            return acc

        def d_send(q):
            return send(mb_part.at[(1 - row) * 2 + q], mb_d2d.at[s, q], md_ss.at[q], md_rs.at[s, q], 1)

        def y_send(q):
            return send(mb_sum.at[q], mb_rcv.at[s, q], my_ss.at[q], my_rs.at[s, q], 4)

        def ga_send():
            return send(ga_snd, ga_rcv.at[s], ga_ss, ga_rs.at[s], 1)

        def reduce_cores(q):
            d_send(q).wait_recv()
            mb_sum[q] = mb_part[row * 2 + q] + mb_d2d[s, q]
            y_send(q).start()

        a_solve(0)
        for jt in range(J_TILES):
            mb_part[jt] = v_tile(jt, 0)
        a_solve(1)
        for n, jt in enumerate((0, 2, 1, 3)):
            mb_part[jt] = mb_part[jt] + v_tile(jt, 1)
            if n == 1:
                ga_snd[...] = sum(dot_nt(at_ref[ch], jnp.concatenate([at_ref[ch], at_ref[ch]], axis=0))
                                  for ch in range(A_CHUNKS))

            @pl.when(row != jt // 2)
            def _():
                d_send(jt % 2).start()

            if n % 2 == 0:
                @pl.when(row == 0)
                def _():
                    reduce_cores(n // 2)
            if n == 1:
                ga_send().start()

        def late_reduce(b):
            if b == 1:
                @pl.when(row == 1)
                def _():
                    reduce_cores(1)

        @pl.when(row == 1)
        def _():
            reduce_cores(0)

        ga_send().wait()
        gram_a = ga_snd[...] + ga_rcv[s]
        inv_b = inverse_quad(gram_a * gram_c, lam, late_reduce)
        g_copies = []

        def b_solve(q):
            y_send(q).wait()
            d_send(q).wait_send()
            b_new = dot_tn(mb_sum[q] + mb_rcv[s, q], inv_b[:RANK], HIGH)
            bo_ref[q] = b_new
            tile = bd.at[s + 1, row * 2 + q]
            tile[...] = b_new.astype(BF16)
            cp = send(tile, tile, ag_ss.at[q], ag_rs.at[s, q], 1)
            cp.start()
            g_copies.append(cp)

        b_solve(0)
        b_solve(1)
        gram_b_start(s)
        u_pass(s + 1, [row * 2, row * 2 + 1], True, False)
        for cp in g_copies:
            cp.wait()
        u_pass(s + 1, [(1 - row) * 2, (1 - row) * 2 + 1], False, True)

        part_c = mc_full[...]
        part_c = part_c + pltpu.roll(part_c, RANK, 1)
        low_c = lax.broadcasted_iota(jnp.int32, (K_LOC // 2, LANES), 1) < RANK
        mc_snd[...] = jnp.where(low_c, part_c[:K_LOC // 2], part_c[K_LOC // 2:])
        for d in (6, 7, 2, 3, 4, 5, 1):
            c_send(s, d).start()
        gram_b_finish(s)
        inv_ref[...] = inverse_quad(gram_a * gb_all[...], lam)
        for d in (1, 2, 3):
            c_send(s, d).wait()
        near = (mc_snd[...] + mc_rcv[s, 0]) + (mc_rcv[s, 1] + mc_rcv[s, 2])
        cd[pl.ds(k_base, K_LOC), :] = c_solve(near)

    c_far(SWEEPS - 1)
    a_rows = a_ref[pl.ds(pl.multiple_of(col * A_CHUNK, A_CHUNK), A_CHUNK), :]
    a_out[...] = jnp.where(tube == 0, a_rows[:, :RANK], a_rows[:, RANK:])
    b_out[...] = bo_ref[tube].T[:RANK]
    c_out[...] = cd[:, :RANK]


def emit(a_in, b_in, c_in, a_hbm, b_hbm, c_hbm, sems):
    pairs = ((b_in, b_hbm), (a_in, a_hbm), (c_in, c_hbm))
    copies = [pltpu.make_async_copy(src, dst, sems.at[n]) for n, (src, dst) in enumerate(pairs)]
    for cp in copies:
        cp.start()
    for cp in copies:
        cp.wait()


def solution(mesh):
    def local(x_blk, b_own, c_full, ridge_lam):
        shapes = ((64, RANK), (RANK, 256), (32, RANK))
        operands = (x_blk, b_own.T, c_full)
        operands = [pltpu.with_memory_space_constraint(v, pltpu.HBM) for v in operands]
        dma = pltpu.SemaphoreType.DMA
        vm = pltpu.VMEM
        a_new, b_new, c_new = pl.pallas_call(
            kernel,
            out_shape=tuple(pltpu.VMEM(shape, F32) for shape in shapes),
            in_specs=[pl.BlockSpec(memory_space=pltpu.HBM)] * 3 + [pl.BlockSpec(memory_space=pltpu.SMEM)],
            out_specs=(pl.BlockSpec(memory_space=pltpu.VMEM),) * 3,
            scratch_shapes=[
                vm((RANK, 256), F32),
                vm((2 * K_LOC, RANK), F32),
                vm((J_TILES, K_LOC, I_LOC, J_TILE), F32),
                vm((J_TILES, K_LOC, I_LOC, J_TILE), BF16),
                vm((K_LOC, I_HALF, LANES), F32),
                vm((SWEEPS + 1, J_TILES, J_TILE, LANES), BF16),
                vm((I_HALF, LANES), BF16),
                vm((3, I_HALF, LANES), BF16),
                vm((2 * K_LOC, LANES), F32),
                vm((K_LOC, RANK, LANES), F32),
                vm((I_HALF, LANES), F32),
                vm((A_CHUNKS, RANK, I_HALF), BF16),
                vm((I_HALF, LANES), F32),
                vm((SWEEPS, 3, I_HALF, LANES), F32),
                vm((RANK, LANES), F32),
                vm((SWEEPS, RANK, LANES), F32),
                vm((J_TILES, RANK, J_TILE), F32),
                vm((SWEEPS, 2, RANK, J_TILE), F32),
                vm((2, RANK, J_TILE), F32),
                vm((SWEEPS, 2, RANK, J_TILE), F32),
                vm((2, J_TILE, LANES), F32),
                vm((RANK // 2, LANES), F32),
                vm((7, RANK // 2, LANES), F32),
                vm((RANK // 2, LANES), F32),
                vm((SWEEPS, 3, RANK // 2, LANES), F32),
                vm((RANK, LANES), F32),
                vm((K_LOC, LANES), F32),
                vm((K_LOC // 2, LANES), F32),
                vm((SWEEPS, 7, K_LOC // 2, LANES), F32),
                vm((LANES, LANES), F32),
                dma((2,)), dma((J_TILES, K_LOC // LOAD_K)), dma((3,)), dma((3,)),
                dma((3, A_CHUNKS)), dma((SWEEPS, 3, A_CHUNKS)),
                dma, dma((SWEEPS,)),
                dma((2,)), dma((SWEEPS, 2)), dma((2,)), dma((SWEEPS, 2)),
                dma((2,)), dma((SWEEPS, 2)),
                dma((7,)), dma((7,)), dma((3,)), dma((SWEEPS, 3)),
                dma((7,)), dma((SWEEPS, 7)),
            ],
            compiler_params=pltpu.CompilerParams(collective_id=0, has_side_effects=True,
                                                 vmem_limit_bytes=52 * 1024 * 1024),
            name="als_sweeps",
        )(*operands, ridge_lam.reshape(1, 1))
        a_new, b_new, c_new = pl.pallas_call(
            emit,
            out_shape=tuple(jax.ShapeDtypeStruct(shape, F32) for shape in shapes),
            in_specs=[pl.BlockSpec(memory_space=pltpu.VMEM)] * 3,
            out_specs=(pl.BlockSpec(memory_space=pl.ANY),) * 3,
            scratch_shapes=[dma((3,))],
            compiler_params=pltpu.CompilerParams(vmem_limit_bytes=1024 * 1024),
            name="emit_factors",
        )(a_new, b_new, c_new)
        return a_new, b_new.T, c_new

    return jax.shard_map(
        local,
        mesh=mesh,
        in_specs=(P("tube", "row", "col"), P(("col", "row", "tube"), None), P(None, None), P()),
        out_specs=(P(("row", "col", "tube"), None), P(("col", "row", "tube"), None), P(None, None)),
        check_vma=False,
    )
```

```python
import functools

import jax
import jax.numpy as jnp
from jax import lax
from jax.experimental import pallas as pl
from jax.experimental.pallas import tpu as pltpu
from jax.sharding import PartitionSpec as P

SWEEPS = 2
RANK = 64
LANES = 128
K_LOC = 16
I_LOC = 256
J_TILE = 256
J_TILES = 4
I_HALF = I_LOC // 2
A_CHUNKS = 2
BLK = 16
LOAD_K = 4
MESH = pl.DeviceIdType.MESH
HIGH = lax.Precision.HIGHEST
F32 = jnp.float32
BF16 = jnp.bfloat16


def dot_nn(a, b, precision=None):
    return lax.dot_general(a, b, (((1,), (0,)), ((), ())), precision=precision, preferred_element_type=F32)


def dot_nt(a, b, precision=None):
    return lax.dot_general(a, b, (((1,), (1,)), ((), ())), precision=precision, preferred_element_type=F32)


def dot_tn(a, b, precision=None):
    return lax.dot_general(a, b, (((0,), (0,)), ((), ())), precision=precision, preferred_element_type=F32)


def spd_inverse(gram_dup, lam, between=None):
    row_ids = lax.broadcasted_iota(jnp.int32, (RANK, LANES), 0)
    lane_ids = lax.broadcasted_iota(jnp.int32, (RANK, LANES), 1)
    left_eye = jnp.where(lane_ids == row_ids, 1.0, 0.0).astype(F32)
    right_eye = jnp.where(lane_ids == row_ids + RANK, 1.0, 0.0).astype(F32)
    aug = jnp.where(lane_ids < RANK, left_eye, gram_dup + lam * right_eye)
    n_blk = RANK // BLK
    blocks = [aug[b * BLK:(b + 1) * BLK] for b in range(n_blk)]
    sub_ids = lax.broadcasted_iota(jnp.int32, (BLK, LANES), 0)

    def lane(block, b, c):
        at = RANK + b * BLK + c
        return jnp.broadcast_to(block[:, at:at + 1], (BLK, LANES))

    def sublane(block, c):
        return jnp.broadcast_to(block[c:c + 1, :], (BLK, LANES))

    done = []
    for b in range(n_blk):
        piv = blocks[b]
        cols = [lane(piv, b, c) for c in range(BLK)]
        mults = [[lane(blocks[t], b, c) for c in range(BLK)] for t in range(b + 1, n_blk)]
        chol_rows = jnp.zeros((BLK, LANES), F32)
        diag = sublane(cols[0], 0)
        for c in range(BLK):
            is_row = sub_ids == c
            root = lax.rsqrt(diag)
            elts = {c2: sublane(cols[c2], c) * root for c2 in range(c + 1, BLK)}
            if c + 1 < BLK:
                diag = sublane(cols[c + 1], c + 1) - (sublane(cols[c], c + 1) * root) * elts[c + 1]
            scaled_col = cols[c] * root
            scaled_row = sublane(piv, c) * root
            chol_rows = jnp.where(is_row, scaled_row, chol_rows)
            piv = jnp.where(is_row, scaled_row * root, piv - scaled_col * scaled_row)
            for c2 in range(c + 1, BLK):
                cols[c2] = jnp.where(is_row, elts[c2] * root, cols[c2] - scaled_col * elts[c2])
        done.append(chol_rows)
        for t in range(b + 1, n_blk):
            upd = blocks[t]
            for c in range(BLK):
                upd = upd - mults[t - b - 1][c] * sublane(piv, c)
            blocks[t] = upd
        if between is not None:
            between(b)
    low_inv = jnp.concatenate(done, axis=0)[:, :RANK]
    return dot_tn(low_inv, low_inv, HIGH)


def kernel(x_hbm, b_hbm, c_hbm, lam_ref, a_out, b_out, c_out,
           b_init, c_init, xf, x4, x4t, u_ref, bt, c_own, c_other, cb, a32_ref, at_ref,
           ma_snd, ma_rcv, ga_snd, ga_rcv, mb_part, mb_d2d, mb_sum, mb_rcv, bo_ref,
           g0_snd, g0_rcv, gb_snd, gb_rcv, gb_all, mc_snd, mc_rcv, inv_ref,
           in_sem, x_sem, b_ss, b_rs, ma_ss, ma_rs, ga_ss, ga_rs, md_ss, md_rs, my_ss, my_rs,
           ag_ss, ag_rs, g0_ss, g0_rs, gb_ss, gb_rs, mc_ss, mc_rs):
    tube, col, row = lax.axis_index("tube"), lax.axis_index("col"), lax.axis_index("row")

    def peer(d):
        t = 1 - tube if d & 4 else tube
        c = 1 - col if d & 2 else col
        r = 1 - row if d & 1 else row
        return (t, c, r)

    def send(src, dst, ss, rs, d):
        return pltpu.make_async_remote_copy(src_ref=src, dst_ref=dst, send_sem=ss, recv_sem=rs,
                                            device_id=peer(d), device_id_type=MESH)

    def load(n, g):
        rows = pl.ds(g * LOAD_K, LOAD_K)
        return pltpu.make_async_copy(x_hbm.at[rows, :, pl.ds(pl.multiple_of(tile_of(n) * J_TILE, J_TILE), J_TILE)],
                                     xf.at[n, rows], x_sem.at[n, g])

    def tile_of(n):
        if n == 0:
            return row * 2 + tube
        if n == 1:
            return (1 - row) * 2 + tube
        return (3 - n) * 2 + 1 - tube

    small = [pltpu.make_async_copy(src, dst, in_sem.at[n])
             for n, (src, dst) in enumerate(((b_hbm, b_init), (c_hbm, c_init)))]
    for cp in small:
        cp.start()

    def load_start(n):
        for g in range(K_LOC // LOAD_K):
            load(n, g).start(priority=1)

    load_start(0)
    load_start(1)
    barrier = pltpu.get_barrier_semaphore()
    for d in range(1, 8):
        pl.semaphore_signal(barrier, inc=1, device_id=peer(d), device_id_type=MESH)

    k_base = pl.multiple_of(tube * K_LOC, K_LOC)
    k_far = pl.multiple_of((1 - tube) * K_LOC, K_LOC)
    lam = lam_ref[0, 0]
    for cp in small:
        cp.wait()
    for n in range(2, J_TILES):
        load_start(n)
    bt[0, row * 2 + tube] = b_init[...].astype(BF16)

    def turn_c(rows):
        wide = jnp.concatenate([rows, jnp.zeros((K_LOC, RANK), F32)], axis=1)
        return jnp.concatenate([wide, jnp.zeros((LANES - K_LOC, LANES), F32)], axis=0).T[:RANK]

    def spread_c():
        for k in range(K_LOC):
            cb[k] = jnp.broadcast_to(c_own[:, k:k + 1], (RANK, LANES))

    c_own[...] = turn_c(c_init[pl.ds(k_base, K_LOC), :])
    c_other[...] = turn_c(c_init[pl.ds(k_far, K_LOC), :])
    pl.semaphore_wait(barrier, 7)

    def b_send(tile, n, d, ss):
        return send(bt.at[0, tile], bt.at[0, tile], b_ss.at[ss], b_rs.at[n - 1], d)

    own_tile = row * 2 + tube

    @pl.when(row == 0)
    def _():
        b_send(own_tile, 3, 4, 1).start()
        b_send(own_tile, 3, 5, 2).start()

    @pl.when(row == 1)
    def _():
        b_send(own_tile, 2, 4, 1).start()

    b_send(own_tile, 1, 1, 0).start()

    half_lanes = lax.broadcasted_iota(jnp.int32, (RANK // 2, LANES), 1) < RANK

    def gram_dup(turned):
        return dot_nt(turned, jnp.concatenate([turned, turned], axis=0))

    def gram_pack(tiles):
        gram = sum(gram_dup(tile) for tile in tiles)
        return jnp.where(half_lanes, gram[:RANK // 2], gram[RANK // 2:])

    def gram_unpack(packed):
        turned = pltpu.roll(packed, RANK, 1)
        return jnp.concatenate([jnp.where(half_lanes, packed, turned), jnp.where(half_lanes, turned, packed)], axis=0)

    def g0_send(d):
        return send(g0_snd, g0_rcv.at[d - 1], g0_ss.at[d - 1], g0_rs.at[d - 1], d)

    def gb_send(s, d):
        return send(gb_snd, gb_rcv.at[s, d - 1], gb_ss.at[d - 1], gb_rs.at[s, d - 1], d)

    def gram_b_start(s):
        gb_snd[...] = gram_pack([bt[s + 1, row * 2], bt[s + 1, row * 2 + 1]])
        for d in (2, 3, 1):
            gb_send(s, d).start()

    def gram_b_finish(s):
        for d in (3, 2, 1):
            gb_send(s, d).wait_recv()
        gb_all[...] = gram_unpack((gb_snd[...] + gb_rcv[s, 0]) + (gb_rcv[s, 1] + gb_rcv[s, 2]))

    lanes_c = lax.broadcasted_iota(jnp.int32, (K_LOC // 2, LANES), 1)

    def u_pass(slot, tiles, first, last, staged=None, slabs=range(K_LOC)):
        packed = jnp.zeros((K_LOC // 2, LANES), F32)
        for k in slabs:
            u_new = jnp.zeros((RANK, I_LOC), F32)
            for jt in tiles:
                if staged is None:
                    x_turn = x4t[jt, k]
                else:
                    x_tile = xf[staged, k].astype(BF16)
                    x4[jt, k] = x_tile
                    x_turn = x_tile.T
                    x4t[jt, k] = x_turn
                u_new = u_new + dot_nn(bt[slot, jt], x_turn)
            if not first:
                u_new = u_ref[k] + u_new
            u_ref[k] = u_new
            if last:
                prod = u_new[:, :I_HALF] * a32_ref[0] + u_new[:, I_HALF:] * a32_ref[1]
                for g in range(RANK // 8):
                    total = jnp.sum(prod[8 * g:8 * g + 8], axis=1, keepdims=True)
                    packed = jnp.where(lanes_c == K_LOC * g + k, total, packed)
        return packed

    g0_snd[...] = gram_pack([bt[0, own_tile]])
    for d in (7, 6, 3, 2, 5, 4, 1):
        g0_send(d).start()
    spread_c()
    for n in range(J_TILES):
        if n > 0:
            b_send(tile_of(n), n, 1, 0).wait_recv()
            if n == 2:
                @pl.when(row == 1)
                def _():
                    b_send(tile_of(2), 2, 1, 2).start()
        step = K_LOC // 2 if n == J_TILES - 1 else K_LOC
        for k in range(0, K_LOC, step):
            for g in range(k // LOAD_K, (k + step) // LOAD_K):
                load(n, g).wait()
            u_pass(0, [tile_of(n)], n == 0, False, staged=n, slabs=range(k, k + step))
    for ss in range(3):
        b_send(own_tile, 1, 1, ss).wait_send()
    for d in range(1, 8):
        g0_send(d).wait()
    here = (g0_snd[...] + g0_rcv[0]) + (g0_rcv[3] + g0_rcv[4])
    there = (g0_rcv[1] + g0_rcv[2]) + (g0_rcv[5] + g0_rcv[6])
    gb_all[...] = gram_unpack(here + there)

    def c_send(s, d):
        return send(mc_snd, mc_rcv.at[s, d - 1], mc_ss.at[d - 1], mc_rs.at[s, d - 1], d)

    def c_solve(packed):
        turned = [packed if g == 0 else pltpu.roll(packed, LANES - K_LOC * g, 1) for g in range(RANK // 8)]
        turned = jnp.concatenate(turned, axis=0)
        lane = lax.broadcasted_iota(jnp.int32, (RANK, LANES), 1)
        return dot_nn(inv_ref[...], jnp.where(lane < K_LOC, turned, 0.0), HIGH)

    def c_sent(s):
        for d in range(1, 8):
            c_send(s, d).wait_send()

    def c_far(s):
        for d in (4, 5, 6, 7):
            c_send(s, d).wait_recv()
        far = (mc_rcv[s, 3] + mc_rcv[s, 4]) + (mc_rcv[s, 5] + mc_rcv[s, 6])
        c_other[...] = c_solve(far)

    @pl.loop(0, SWEEPS)
    def _(s):
        def a_send(ch, d):
            n = d // 2 - 1
            return send(ma_snd.at[ch], ma_rcv.at[s, n, ch], ma_ss.at[n, ch], ma_rs.at[s, n, ch], d)

        for ch in range(A_CHUNKS):
            part = jnp.zeros((RANK, I_HALF), F32)
            for k in range(K_LOC):
                part = part + u_ref[k, :, ch * I_HALF:(ch + 1) * I_HALF] * cb[k]
            ma_snd[ch] = part
            for d in (6, 4, 2):
                a_send(ch, d).start()

        @pl.when(s > 0)
        def _():
            c_far(s - 1)

        gram_c = gram_dup(c_own[...].astype(BF16)) + gram_dup(c_other[...].astype(BF16))
        inv_a = spd_inverse(gb_all[...] * gram_c, lam)
        def a_solve(ch):
            for d in (2, 4, 6):
                a_send(ch, d).wait_recv()
            mtt_a = (ma_snd[ch] + ma_rcv[s, 0, ch]) + (ma_rcv[s, 1, ch] + ma_rcv[s, 2, ch])
            a_turn = dot_nn(inv_a, mtt_a, HIGH)
            a32_ref[ch] = a_turn
            at_ref[ch] = a_turn.astype(BF16)

        def v_tile(jt, ch):
            acc = jnp.zeros((RANK, J_TILE), F32)
            for k in range(K_LOC):
                v_kt = dot_nn(at_ref[ch], x4[jt, k, ch * I_HALF:(ch + 1) * I_HALF, :])
                c_col = cb[k]
                acc = acc + v_kt * jnp.concatenate([c_col, c_col], axis=1)
            return acc

        def d_send(q):
            return send(mb_part.at[(1 - row) * 2 + q], mb_d2d.at[s, q], md_ss.at[q], md_rs.at[s, q], 1)

        def y_send(q):
            return send(mb_sum.at[q], mb_rcv.at[s, q], my_ss.at[q], my_rs.at[s, q], 4)

        def ga_send():
            return send(ga_snd, ga_rcv.at[s], ga_ss, ga_rs.at[s], 1)

        def reduce_cores(q):
            d_send(q).wait_recv()
            mb_sum[q] = mb_part[row * 2 + q] + mb_d2d[s, q]
            y_send(q).start()

        a_solve(0)
        for jt in range(J_TILES):
            mb_part[jt] = v_tile(jt, 0)
        a_solve(1)

        def v_last(jt):
            mb_part[jt] = mb_part[jt] + v_tile(jt, 1)

        v_last(0)

        @pl.when(row == 0)
        def _():
            reduce_cores(0)

        @pl.when(row == 1)
        def _():
            d_send(0).start()

        v_last(2)
        ga_snd[...] = sum(gram_dup(at_ref[ch]) for ch in range(A_CHUNKS))

        @pl.when(row == 0)
        def _():
            d_send(0).start()

        ga_send().start()
        v_last(1)
        v_last(3)

        @pl.when(row == 0)
        def _():
            reduce_cores(1)

        d_send(1).start()

        def late_reduce(b):
            if b == 0:
                @pl.when(row == 1)
                def _():
                    reduce_cores(1)

        @pl.when(row == 1)
        def _():
            reduce_cores(0)

        ga_send().wait_recv()
        gram_a = ga_snd[...] + ga_rcv[s]
        inv_b = spd_inverse(gram_a * gram_c, lam, late_reduce)
        g_copies = []

        def b_solve(q):
            y_send(q).wait_recv()
            b_new = dot_nn(inv_b, mb_sum[q] + mb_rcv[s, q], HIGH)
            bo_ref[q] = b_new
            tile = bt.at[s + 1, row * 2 + q]
            tile[...] = b_new.astype(BF16)
            cp = send(tile, tile, ag_ss.at[q], ag_rs.at[s, q], 1)
            cp.start()
            g_copies.append(cp)

        b_solve(0)
        b_solve(1)
        gram_b_start(s)
        u_pass(s + 1, [row * 2, row * 2 + 1], True, False)
        for cp in g_copies:
            cp.wait_recv()
        part_c = u_pass(s + 1, [(1 - row) * 2, (1 - row) * 2 + 1], False, True)

        @pl.when(s > 0)
        def _():
            c_sent(s - 1)

        mc_snd[...] = part_c
        for d in (6, 7, 2, 3, 4, 5, 1):
            c_send(s, d).start()
        gram_b_finish(s)
        inv_ref[...] = spd_inverse(gram_a * gb_all[...], lam)
        for ch in range(A_CHUNKS):
            for d in (2, 4, 6):
                a_send(ch, d).wait_send()
        ga_send().wait_send()
        for q in range(2):
            d_send(q).wait_send()
            y_send(q).wait_send()
            g_copies[q].wait_send()
        for d in (1, 2, 3):
            gb_send(s, d).wait_send()
        for d in (1, 2, 3):
            c_send(s, d).wait_recv()
        near = (mc_snd[...] + mc_rcv[s, 0]) + (mc_rcv[s, 1] + mc_rcv[s, 2])
        c_own[...] = c_solve(near)
        spread_c()

    c_far(SWEEPS - 1)
    c_sent(SWEEPS - 1)
    a_rows = a32_ref[col].T
    a_out[...] = jnp.where(tube == 0, a_rows[:I_HALF // 2], a_rows[I_HALF // 2:])
    b_out[...] = bo_ref[tube]
    c_out[pl.ds(k_base, K_LOC), :] = c_own[...].T[:K_LOC]
    c_out[pl.ds(k_far, K_LOC), :] = c_other[...].T[:K_LOC]


def emit(a_in, b_in, c_in, a_hbm, b_hbm, c_hbm, sems):
    pairs = ((b_in, b_hbm), (a_in, a_hbm), (c_in, c_hbm))
    copies = [pltpu.make_async_copy(src, dst, sems.at[n]) for n, (src, dst) in enumerate(pairs)]
    for cp in copies:
        cp.start()
    for cp in copies:
        cp.wait()


def solution(mesh):
    def local(x_blk, b_own, c_full, ridge_lam):
        shapes = ((64, RANK), (RANK, 256), (32, RANK))
        operands = (x_blk, b_own.T, c_full)
        operands = [pltpu.with_memory_space_constraint(v, pltpu.HBM) for v in operands]
        dma = pltpu.SemaphoreType.DMA
        vm = pltpu.VMEM
        a_new, b_new, c_new = pl.pallas_call(
            kernel,
            out_shape=tuple(pltpu.VMEM(shape, F32) for shape in shapes),
            in_specs=[pl.BlockSpec(memory_space=pltpu.HBM)] * 3 + [pl.BlockSpec(memory_space=pltpu.SMEM)],
            out_specs=(pl.BlockSpec(memory_space=pltpu.VMEM),) * 3,
            scratch_shapes=[
                vm((RANK, J_TILE), F32),
                vm((2 * K_LOC, RANK), F32),
                vm((J_TILES, K_LOC, I_LOC, J_TILE), F32),
                vm((J_TILES, K_LOC, I_LOC, J_TILE), BF16),
                vm((J_TILES, K_LOC, J_TILE, I_LOC), BF16),
                vm((K_LOC, RANK, I_LOC), F32),
                vm((SWEEPS + 1, J_TILES, RANK, J_TILE), BF16),
                vm((RANK, LANES), F32),
                vm((RANK, LANES), F32),
                vm((K_LOC, RANK, LANES), F32),
                vm((A_CHUNKS, RANK, I_HALF), F32),
                vm((A_CHUNKS, RANK, I_HALF), BF16),
                vm((A_CHUNKS, RANK, I_HALF), F32),
                vm((SWEEPS, 3, A_CHUNKS, RANK, I_HALF), F32),
                vm((RANK, LANES), F32),
                vm((SWEEPS, RANK, LANES), F32),
                vm((J_TILES, RANK, J_TILE), F32),
                vm((SWEEPS, 2, RANK, J_TILE), F32),
                vm((2, RANK, J_TILE), F32),
                vm((SWEEPS, 2, RANK, J_TILE), F32),
                vm((2, RANK, J_TILE), F32),
                vm((RANK // 2, LANES), F32),
                vm((7, RANK // 2, LANES), F32),
                vm((RANK // 2, LANES), F32),
                vm((SWEEPS, 3, RANK // 2, LANES), F32),
                vm((RANK, LANES), F32),
                vm((K_LOC // 2, LANES), F32),
                vm((SWEEPS, 7, K_LOC // 2, LANES), F32),
                vm((RANK, RANK), F32),
                dma((2,)), dma((J_TILES, K_LOC // LOAD_K)), dma((3,)), dma((3,)),
                dma((3, A_CHUNKS)), dma((SWEEPS, 3, A_CHUNKS)),
                dma, dma((SWEEPS,)),
                dma((2,)), dma((SWEEPS, 2)), dma((2,)), dma((SWEEPS, 2)),
                dma((2,)), dma((SWEEPS, 2)),
                dma((7,)), dma((7,)), dma((3,)), dma((SWEEPS, 3)),
                dma((7,)), dma((SWEEPS, 7)),
            ],
            compiler_params=pltpu.CompilerParams(collective_id=0, has_side_effects=True,
                                                 vmem_limit_bytes=52 * 1024 * 1024),
            name="als_sweeps",
        )(*operands, ridge_lam.reshape(1, 1))
        a_new, b_new, c_new = pl.pallas_call(
            emit,
            out_shape=tuple(jax.ShapeDtypeStruct(shape, F32) for shape in shapes),
            in_specs=[pl.BlockSpec(memory_space=pltpu.VMEM)] * 3,
            out_specs=(pl.BlockSpec(memory_space=pl.ANY),) * 3,
            scratch_shapes=[dma((3,))],
            compiler_params=pltpu.CompilerParams(vmem_limit_bytes=1024 * 1024),
            name="emit_factors",
        )(a_new, b_new, c_new)
        return a_new, b_new.T, c_new

    return jax.shard_map(
        local,
        mesh=mesh,
        in_specs=(P("tube", "row", "col"), P(("col", "row", "tube"), None), P(None, None), P()),
        out_specs=(P(("row", "col", "tube"), None), P(("col", "row", "tube"), None), P(None, None)),
        check_vma=False,
    )
```

```python
import functools

import jax
import jax.numpy as jnp
from jax import lax
from jax.experimental import pallas as pl
from jax.experimental.pallas import tpu as pltpu
from jax.sharding import PartitionSpec as P

SWEEPS = 2
RANK = 64
LANES = 128
K_LOC = 16
I_LOC = 256
J_TILE = 256
J_TILES = 4
I_HALF = I_LOC // 2
A_CHUNKS = 2
BLK = 16
LOAD_K = 4
MESH = pl.DeviceIdType.MESH
HIGH = lax.Precision.HIGHEST
F32 = jnp.float32
BF16 = jnp.bfloat16


def dot_nn(a, b, precision=None):
    return lax.dot_general(a, b, (((1,), (0,)), ((), ())), precision=precision, preferred_element_type=F32)


def dot_nt(a, b, precision=None):
    return lax.dot_general(a, b, (((1,), (1,)), ((), ())), precision=precision, preferred_element_type=F32)


def dot_tn(a, b, precision=None):
    return lax.dot_general(a, b, (((0,), (0,)), ((), ())), precision=precision, preferred_element_type=F32)


def spd_inverse(gram_dup, lam, between=None):
    row_ids = lax.broadcasted_iota(jnp.int32, (RANK, LANES), 0)
    lane_ids = lax.broadcasted_iota(jnp.int32, (RANK, LANES), 1)
    left_eye = jnp.where(lane_ids == row_ids, 1.0, 0.0).astype(F32)
    right_eye = jnp.where(lane_ids == row_ids + RANK, 1.0, 0.0).astype(F32)
    aug = jnp.where(lane_ids < RANK, left_eye, gram_dup + lam * right_eye)
    n_blk = RANK // BLK
    blocks = [aug[b * BLK:(b + 1) * BLK] for b in range(n_blk)]
    sub_ids = lax.broadcasted_iota(jnp.int32, (BLK, LANES), 0)

    def lane(block, b, c):
        at = RANK + b * BLK + c
        return jnp.broadcast_to(block[:, at:at + 1], (BLK, LANES))

    def sublane(block, c):
        return jnp.broadcast_to(block[c:c + 1, :], (BLK, LANES))

    done = []
    for b in range(n_blk):
        piv = blocks[b]
        cols = [lane(piv, b, c) for c in range(BLK)]
        mults = [[lane(blocks[t], b, c) for c in range(BLK)] for t in range(b + 1, n_blk)]
        chol_rows = jnp.zeros((BLK, LANES), F32)
        diag = sublane(cols[0], 0)
        for c in range(BLK):
            is_row = sub_ids == c
            root = lax.rsqrt(diag)
            elts = {c2: sublane(cols[c2], c) * root for c2 in range(c + 1, BLK)}
            if c + 1 < BLK:
                diag = sublane(cols[c + 1], c + 1) - (sublane(cols[c], c + 1) * root) * elts[c + 1]
            scaled_col = cols[c] * root
            scaled_row = sublane(piv, c) * root
            chol_rows = jnp.where(is_row, scaled_row, chol_rows)
            piv = jnp.where(is_row, scaled_row * root, piv - scaled_col * scaled_row)
            for c2 in range(c + 1, BLK):
                cols[c2] = jnp.where(is_row, elts[c2] * root, cols[c2] - scaled_col * elts[c2])
        done.append(chol_rows)
        for t in range(b + 1, n_blk):
            upd = blocks[t]
            for c in range(BLK):
                upd = upd - mults[t - b - 1][c] * sublane(piv, c)
            blocks[t] = upd
        if between is not None:
            between(b)
    low_inv = jnp.concatenate(done, axis=0)[:, :RANK]
    return dot_tn(low_inv, low_inv, HIGH)


def kernel(x_hbm, b_hbm, c_hbm, lam_ref, a_out, b_out, c_out,
           b_init, c_init, xf, x4, x4t, u_ref, bt, c_own, c_other, cb, a32_ref, at_ref,
           ma_snd, ma_rcv, ga_snd, ga_rcv, mb_part, mb_d2d, mb_sum, mb_rcv, bo_ref,
           g0_snd, g0_rcv, gb_part, gb_snd, gb_rcv, gb_all, mc_snd, mc_rcv, inv_ref,
           in_sem, x_sem, b_ss, b_rs, ma_ss, ma_rs, ga_ss, ga_rs, md_ss, md_rs, my_ss, my_rs,
           ag_ss, ag_rs, g0_ss, g0_rs, gb_ss, gb_rs, mc_ss, mc_rs):
    tube, col, row = lax.axis_index("tube"), lax.axis_index("col"), lax.axis_index("row")

    def peer(d):
        t = 1 - tube if d & 4 else tube
        c = 1 - col if d & 2 else col
        r = 1 - row if d & 1 else row
        return (t, c, r)

    def send(src, dst, ss, rs, d):
        return pltpu.make_async_remote_copy(src_ref=src, dst_ref=dst, send_sem=ss, recv_sem=rs,
                                            device_id=peer(d), device_id_type=MESH)

    def load(n, g):
        rows = pl.ds(g * LOAD_K, LOAD_K)
        return pltpu.make_async_copy(x_hbm.at[rows, :, pl.ds(pl.multiple_of(tile_of(n) * J_TILE, J_TILE), J_TILE)],
                                     xf.at[n, rows], x_sem.at[n, g])

    def tile_of(n):
        if n == 0:
            return row * 2 + tube
        if n == 1:
            return (1 - row) * 2 + tube
        return (3 - n) * 2 + 1 - tube

    small = [pltpu.make_async_copy(src, dst, in_sem.at[n])
             for n, (src, dst) in enumerate(((b_hbm, b_init), (c_hbm, c_init)))]
    for cp in small:
        cp.start()

    def load_start(n):
        for g in range(K_LOC // LOAD_K):
            load(n, g).start(priority=1)

    load_start(0)
    load_start(1)
    barrier = pltpu.get_barrier_semaphore()
    for d in range(1, 8):
        pl.semaphore_signal(barrier, inc=1, device_id=peer(d), device_id_type=MESH)

    k_base = pl.multiple_of(tube * K_LOC, K_LOC)
    k_far = pl.multiple_of((1 - tube) * K_LOC, K_LOC)
    lam = lam_ref[0, 0]
    for cp in small:
        cp.wait()
    for n in range(2, J_TILES):
        load_start(n)
    bt[0, row * 2 + tube] = b_init[...].astype(BF16)

    def turn_c(rows):
        wide = jnp.concatenate([rows, jnp.zeros((K_LOC, RANK), F32)], axis=1)
        return jnp.concatenate([wide, jnp.zeros((LANES - K_LOC, LANES), F32)], axis=0).T[:RANK]

    def spread_c():
        for k in range(K_LOC):
            cb[k] = jnp.broadcast_to(c_own[:, k:k + 1], (RANK, LANES))

    c_own[...] = turn_c(c_init[pl.ds(k_base, K_LOC), :])
    c_other[...] = turn_c(c_init[pl.ds(k_far, K_LOC), :])
    pl.semaphore_wait(barrier, 7)

    def b_send(tile, n, d, ss):
        return send(bt.at[0, tile], bt.at[0, tile], b_ss.at[ss], b_rs.at[n - 1], d)

    own_tile = row * 2 + tube

    @pl.when(row == 0)
    def _():
        b_send(own_tile, 3, 4, 1).start()
        b_send(own_tile, 3, 5, 2).start()

    @pl.when(row == 1)
    def _():
        b_send(own_tile, 2, 4, 1).start()

    b_send(own_tile, 1, 1, 0).start()

    half_lanes = lax.broadcasted_iota(jnp.int32, (RANK // 2, LANES), 1) < RANK

    def gram_dup(turned):
        return dot_nt(turned, jnp.concatenate([turned, turned], axis=0))

    def gram_pack(tiles):
        gram = sum(gram_dup(tile) for tile in tiles)
        return jnp.where(half_lanes, gram[:RANK // 2], gram[RANK // 2:])

    def gram_unpack(packed):
        turned = pltpu.roll(packed, RANK, 1)
        return jnp.concatenate([jnp.where(half_lanes, packed, turned), jnp.where(half_lanes, turned, packed)], axis=0)

    def g0_send(d):
        return send(g0_snd, g0_rcv.at[d - 1], g0_ss.at[d - 1], g0_rs.at[d - 1], d)

    def gb_send(s, d):
        return send(gb_snd, gb_rcv.at[s, d - 1], gb_ss.at[d - 1], gb_rs.at[s, d - 1], d)

    def gram_b_start(s):
        gb_snd[...] = gb_part[...] + gram_pack([bt[s + 1, row * 2 + 1]])
        for core in range(2):
            n = 1 + (row if core == 0 else 1 - row)
            pltpu.make_async_remote_copy(src_ref=gb_snd, dst_ref=gb_rcv.at[s, n], send_sem=gb_ss.at[n],
                                         recv_sem=gb_rs.at[s, n], device_id=(tube, 1 - col, core),
                                         device_id_type=MESH).start()
        gb_send(s, 1).start()

    def gram_b_finish(s):
        for d in (3, 2, 1):
            gb_send(s, d).wait_recv()
        gb_all[...] = gram_unpack((gb_snd[...] + gb_rcv[s, 0]) + (gb_rcv[s, 1] + gb_rcv[s, 2]))

    lanes_c = lax.broadcasted_iota(jnp.int32, (K_LOC // 2, LANES), 1)

    def u_pass(slot, tiles, first, last, staged=None, slabs=range(K_LOC)):
        packed = jnp.zeros((K_LOC // 2, LANES), F32)
        for k in slabs:
            u_new = jnp.zeros((RANK, I_LOC), F32)
            for jt in tiles:
                if staged is None:
                    x_turn = x4t[jt, k]
                else:
                    x_tile = xf[staged, k].astype(BF16)
                    x4[jt, k] = x_tile
                    x_turn = x_tile.T
                    x4t[jt, k] = x_turn
                u_new = u_new + dot_nn(bt[slot, jt], x_turn)
            if not first:
                u_new = u_ref[k] + u_new
            u_ref[k] = u_new
            if last:
                prod = u_new[:, :I_HALF] * a32_ref[0] + u_new[:, I_HALF:] * a32_ref[1]
                for g in range(RANK // 8):
                    total = jnp.sum(prod[8 * g:8 * g + 8], axis=1, keepdims=True)
                    packed = jnp.where(lanes_c == K_LOC * g + k, total, packed)
        return packed

    g0_snd[...] = gram_pack([bt[0, own_tile]])
    for d in (7, 6, 3, 2, 5, 4, 1):
        g0_send(d).start()
    spread_c()
    for n in range(J_TILES):
        if n > 0:
            b_send(tile_of(n), n, 1, 0).wait_recv()
            if n == 2:
                @pl.when(row == 1)
                def _():
                    b_send(tile_of(2), 2, 1, 2).start()
        step = K_LOC // 2 if n == J_TILES - 1 else K_LOC
        for k in range(0, K_LOC, step):
            for g in range(k // LOAD_K, (k + step) // LOAD_K):
                load(n, g).wait()
            u_pass(0, [tile_of(n)], n == 0, False, staged=n, slabs=range(k, k + step))
    for ss in range(3):
        b_send(own_tile, 1, 1, ss).wait_send()
    for d in range(1, 8):
        g0_send(d).wait()
    here = (g0_snd[...] + g0_rcv[0]) + (g0_rcv[3] + g0_rcv[4])
    there = (g0_rcv[1] + g0_rcv[2]) + (g0_rcv[5] + g0_rcv[6])
    gb_all[...] = gram_unpack(here + there)

    def c_send(s, d):
        return send(mc_snd, mc_rcv.at[s, d - 1], mc_ss.at[d - 1], mc_rs.at[s, d - 1], d)

    def c_solve(packed):
        turned = [packed if g == 0 else pltpu.roll(packed, LANES - K_LOC * g, 1) for g in range(RANK // 8)]
        turned = jnp.concatenate(turned, axis=0)
        lane = lax.broadcasted_iota(jnp.int32, (RANK, LANES), 1)
        return dot_nn(inv_ref[...], jnp.where(lane < K_LOC, turned, 0.0), HIGH)

    def c_sent(s):
        for d in range(1, 8):
            c_send(s, d).wait_send()

    def c_near(s):
        c_own[...] = c_solve((mc_snd[...] + mc_rcv[s, 0]) + (mc_rcv[s, 1] + mc_rcv[s, 2]))

    def c_far(s):
        c_other[...] = c_solve((mc_rcv[s, 3] + mc_rcv[s, 4]) + (mc_rcv[s, 5] + mc_rcv[s, 6]))

    def c_far_wait(s):
        for d in (4, 5, 6, 7):
            c_send(s, d).wait_recv()

    @pl.loop(0, SWEEPS)
    def _(s):
        def a_send(ch, d):
            n = d // 2 - 1
            return send(ma_snd.at[ch], ma_rcv.at[s, n, ch], ma_ss.at[n, ch], ma_rs.at[s, n, ch], d)

        for ch in range(A_CHUNKS):
            part = jnp.zeros((RANK, I_HALF), F32)
            for k in range(K_LOC):
                part = part + u_ref[k, :, ch * I_HALF:(ch + 1) * I_HALF] * cb[k]
            ma_snd[ch] = part
            for d in (6, 4, 2):
                a_send(ch, d).start()

        @pl.when(s > 0)
        def _():
            c_far_wait(s - 1)
            c_far(s - 1)

        gram_c = gram_dup(c_own[...].astype(BF16)) + gram_dup(c_other[...].astype(BF16))
        inv_a = spd_inverse(gb_all[...] * gram_c, lam)
        def a_solve(ch):
            for d in (2, 4, 6):
                a_send(ch, d).wait_recv()
            mtt_a = (ma_snd[ch] + ma_rcv[s, 0, ch]) + (ma_rcv[s, 1, ch] + ma_rcv[s, 2, ch])
            a_turn = dot_nn(inv_a, mtt_a, HIGH)
            a32_ref[ch] = a_turn
            at_ref[ch] = a_turn.astype(BF16)

        def v_tile(jt, ch):
            acc = jnp.zeros((RANK, J_TILE), F32)
            for k in range(K_LOC):
                v_kt = dot_nn(at_ref[ch], x4[jt, k, ch * I_HALF:(ch + 1) * I_HALF, :])
                c_col = cb[k]
                acc = acc + v_kt * jnp.concatenate([c_col, c_col], axis=1)
            return acc

        def d_send(q):
            return send(mb_part.at[(1 - row) * 2 + q], mb_d2d.at[s, q], md_ss.at[q], md_rs.at[s, q], 1)

        def y_send(q):
            return send(mb_sum.at[q], mb_rcv.at[s, q], my_ss.at[q], my_rs.at[s, q], 4)

        def ga_send():
            return send(ga_snd, ga_rcv.at[s], ga_ss, ga_rs.at[s], 1)

        def reduce_cores(q):
            d_send(q).wait_recv()
            mb_sum[q] = mb_part[row * 2 + q] + mb_d2d[s, q]
            y_send(q).start()

        a_solve(0)
        for jt in range(J_TILES):
            mb_part[jt] = v_tile(jt, 0)
        a_solve(1)

        def v_last(jt):
            mb_part[jt] = mb_part[jt] + v_tile(jt, 1)

        v_last(0)

        @pl.when(row == 0)
        def _():
            reduce_cores(0)

        @pl.when(row == 1)
        def _():
            d_send(0).start()

        v_last(2)
        ga_snd[...] = sum(gram_dup(at_ref[ch]) for ch in range(A_CHUNKS))

        @pl.when(row == 0)
        def _():
            d_send(0).start()

        ga_send().start()
        v_last(1)
        v_last(3)

        @pl.when(row == 0)
        def _():
            reduce_cores(1)

        d_send(1).start()

        def late_reduce(b):
            if b == 0:
                @pl.when(row == 1)
                def _():
                    reduce_cores(1)

        @pl.when(row == 1)
        def _():
            reduce_cores(0)

        ga_send().wait_recv()
        gram_a = ga_snd[...] + ga_rcv[s]
        inv_b = spd_inverse(gram_a * gram_c, lam, late_reduce)
        g_copies = []

        def b_solve(q):
            y_send(q).wait_recv()
            b_new = dot_nn(inv_b, mb_sum[q] + mb_rcv[s, q], HIGH)
            bo_ref[q] = b_new
            tile = bt.at[s + 1, row * 2 + q]
            tile[...] = b_new.astype(BF16)
            cp = send(tile, tile, ag_ss.at[q], ag_rs.at[s, q], 1)
            cp.start()
            g_copies.append(cp)

        b_solve(0)
        gb_part[...] = gram_pack([bt[s + 1, row * 2]])
        b_solve(1)
        gram_b_start(s)
        u_pass(s + 1, [row * 2, row * 2 + 1], True, False)
        g_copies[0].wait_recv()
        u_pass(s + 1, [(1 - row) * 2], False, False)
        g_copies[1].wait_recv()
        part_c = u_pass(s + 1, [(1 - row) * 2 + 1], False, True)

        @pl.when(s > 0)
        def _():
            c_sent(s - 1)

        mc_snd[...] = part_c
        for d in (6, 7, 2, 3, 4, 5, 1):
            c_send(s, d).start()
        a_rows = a32_ref[col].T
        a_out[...] = jnp.where(tube == 0, a_rows[:I_HALF // 2], a_rows[I_HALF // 2:])
        b_out[...] = bo_ref[tube]
        gram_b_finish(s)
        inv_ref[...] = spd_inverse(gram_a * gb_all[...], lam)
        for ch in range(A_CHUNKS):
            for d in (2, 4, 6):
                a_send(ch, d).wait_send()
        ga_send().wait_send()
        for q in range(2):
            d_send(q).wait_send()
            y_send(q).wait_send()
            g_copies[q].wait_send()
        for d in (1, 2, 3):
            gb_send(s, d).wait_send()
        for d in (1, 2, 3):
            c_send(s, d).wait_recv()

        @pl.when(s < SWEEPS - 1)
        def _():
            c_near(s)
            spread_c()

    c_far_wait(SWEEPS - 1)
    c_near(SWEEPS - 1)
    c_far(SWEEPS - 1)
    c_sent(SWEEPS - 1)
    c_out[pl.ds(k_base, K_LOC), :] = c_own[...].T[:K_LOC]
    c_out[pl.ds(k_far, K_LOC), :] = c_other[...].T[:K_LOC]


def emit(a_in, b_in, c_in, a_hbm, b_hbm, c_hbm, sems):
    pairs = ((b_in, b_hbm), (a_in, a_hbm), (c_in, c_hbm))
    copies = [pltpu.make_async_copy(src, dst, sems.at[n]) for n, (src, dst) in enumerate(pairs)]
    for cp in copies:
        cp.start()
    for cp in copies:
        cp.wait()


def solution(mesh):
    def local(x_blk, b_own, c_full, ridge_lam):
        shapes = ((64, RANK), (RANK, 256), (32, RANK))
        operands = (x_blk, b_own.T, c_full)
        operands = [pltpu.with_memory_space_constraint(v, pltpu.HBM) for v in operands]
        dma = pltpu.SemaphoreType.DMA
        vm = pltpu.VMEM
        a_new, b_new, c_new = pl.pallas_call(
            kernel,
            out_shape=tuple(pltpu.VMEM(shape, F32) for shape in shapes),
            in_specs=[pl.BlockSpec(memory_space=pltpu.HBM)] * 3 + [pl.BlockSpec(memory_space=pltpu.SMEM)],
            out_specs=(pl.BlockSpec(memory_space=pltpu.VMEM),) * 3,
            scratch_shapes=[
                vm((RANK, J_TILE), F32),
                vm((2 * K_LOC, RANK), F32),
                vm((J_TILES, K_LOC, I_LOC, J_TILE), F32),
                vm((J_TILES, K_LOC, I_LOC, J_TILE), BF16),
                vm((J_TILES, K_LOC, J_TILE, I_LOC), BF16),
                vm((K_LOC, RANK, I_LOC), F32),
                vm((SWEEPS + 1, J_TILES, RANK, J_TILE), BF16),
                vm((RANK, LANES), F32),
                vm((RANK, LANES), F32),
                vm((K_LOC, RANK, LANES), F32),
                vm((A_CHUNKS, RANK, I_HALF), F32),
                vm((A_CHUNKS, RANK, I_HALF), BF16),
                vm((A_CHUNKS, RANK, I_HALF), F32),
                vm((SWEEPS, 3, A_CHUNKS, RANK, I_HALF), F32),
                vm((RANK, LANES), F32),
                vm((SWEEPS, RANK, LANES), F32),
                vm((J_TILES, RANK, J_TILE), F32),
                vm((SWEEPS, 2, RANK, J_TILE), F32),
                vm((2, RANK, J_TILE), F32),
                vm((SWEEPS, 2, RANK, J_TILE), F32),
                vm((2, RANK, J_TILE), F32),
                vm((RANK // 2, LANES), F32),
                vm((7, RANK // 2, LANES), F32),
                vm((RANK // 2, LANES), F32),
                vm((RANK // 2, LANES), F32),
                vm((SWEEPS, 3, RANK // 2, LANES), F32),
                vm((RANK, LANES), F32),
                vm((K_LOC // 2, LANES), F32),
                vm((SWEEPS, 7, K_LOC // 2, LANES), F32),
                vm((RANK, RANK), F32),
                dma((2,)), dma((J_TILES, K_LOC // LOAD_K)), dma((3,)), dma((3,)),
                dma((3, A_CHUNKS)), dma((SWEEPS, 3, A_CHUNKS)),
                dma, dma((SWEEPS,)),
                dma((2,)), dma((SWEEPS, 2)), dma((2,)), dma((SWEEPS, 2)),
                dma((2,)), dma((SWEEPS, 2)),
                dma((7,)), dma((7,)), dma((3,)), dma((SWEEPS, 3)),
                dma((7,)), dma((SWEEPS, 7)),
            ],
            compiler_params=pltpu.CompilerParams(collective_id=0, has_side_effects=True,
                                                 vmem_limit_bytes=52 * 1024 * 1024),
            name="als_sweeps",
        )(*operands, ridge_lam.reshape(1, 1))
        a_new, b_new, c_new = pl.pallas_call(
            emit,
            out_shape=tuple(jax.ShapeDtypeStruct(shape, F32) for shape in shapes),
            in_specs=[pl.BlockSpec(memory_space=pltpu.VMEM)] * 3,
            out_specs=(pl.BlockSpec(memory_space=pl.ANY),) * 3,
            scratch_shapes=[dma((3,))],
            compiler_params=pltpu.CompilerParams(vmem_limit_bytes=1024 * 1024),
            name="emit_factors",
        )(a_new, b_new, c_new)
        return a_new, b_new.T, c_new

    return jax.shard_map(
        local,
        mesh=mesh,
        in_specs=(P("tube", "row", "col"), P(("col", "row", "tube"), None), P(None, None), P()),
        out_specs=(P(("row", "col", "tube"), None), P(("col", "row", "tube"), None), P(None, None)),
        check_vma=False,
    )
```

```python
import jax
import jax.numpy as jnp
from jax import lax
from jax.experimental import pallas as pl
from jax.experimental.pallas import tpu as pltpu
from jax.sharding import PartitionSpec as P

SWEEPS = 2
RANK = 64
LANES = 128
K_LOC = 16
I_LOC = 256
J_TILE = 256
J_TILES = 4
I_HALF = I_LOC // 2
A_CHUNKS = 2
BLK = 16
SUB = 8
LOAD_K = 4
MESH = pl.DeviceIdType.MESH
HIGH = lax.Precision.HIGHEST
F32 = jnp.float32
BF16 = jnp.bfloat16


def dot_nn(a, b, precision=None):
    return lax.dot_general(a, b, (((1,), (0,)), ((), ())), precision=precision, preferred_element_type=F32)


def dot_nt(a, b, precision=None):
    return lax.dot_general(a, b, (((1,), (1,)), ((), ())), precision=precision, preferred_element_type=F32)


def dot_tn(a, b, precision=None):
    return lax.dot_general(a, b, (((0,), (0,)), ((), ())), precision=precision, preferred_element_type=F32)


def spd_inverse(gram_dup, lam, between=None):
    row_ids = lax.broadcasted_iota(jnp.int32, (RANK, LANES), 0)
    lane_ids = lax.broadcasted_iota(jnp.int32, (RANK, LANES), 1)
    left_eye = jnp.where(lane_ids == row_ids, 1.0, 0.0).astype(F32)
    right_eye = jnp.where(lane_ids == row_ids + RANK, 1.0, 0.0).astype(F32)
    aug = jnp.where(lane_ids < RANK, left_eye, gram_dup + lam * right_eye)
    groups = [aug[n * SUB:(n + 1) * SUB] for n in range(RANK // SUB)]
    sub_ids = lax.broadcasted_iota(jnp.int32, (SUB, LANES), 0)
    per_blk = BLK // SUB

    def lane(group, at):
        return jnp.broadcast_to(group[:, at:at + 1], (SUB, LANES))

    def sublane(parts, c):
        part = parts[c // SUB]
        return jnp.broadcast_to(part[c % SUB:c % SUB + 1, :], (SUB, LANES))

    done = []
    for b in range(RANK // BLK):
        first, start = b * per_blk, RANK + b * BLK
        piv = groups[first:first + per_blk]
        cols = [[lane(part, start + c) for part in piv] for c in range(BLK)]
        rest = range(first + per_blk, RANK // SUB)
        mults = {n: [lane(groups[n], start + c) for c in range(BLK)] for n in rest}
        chol_rows = [jnp.zeros((SUB, LANES), F32) for _ in range(per_blk)]
        diag = sublane(cols[0], 0)
        for c in range(BLK):
            is_row = sub_ids == c % SUB
            home = c // SUB
            root = lax.rsqrt(diag)
            elts = {c2: sublane(cols[c2], c) * root for c2 in range(c + 1, BLK)}
            if c + 1 < BLK:
                diag = sublane(cols[c + 1], c + 1) - (sublane(cols[c], c + 1) * root) * elts[c + 1]
            scaled_col = [part * root for part in cols[c]]
            scaled_row = sublane(piv, c) * root

            def eliminate(parts, elt):
                new = [part - scale * elt for part, scale in zip(parts, scaled_col)]
                new[home] = jnp.where(is_row, elt * root, new[home])
                return new

            chol_rows[home] = jnp.where(is_row, scaled_row, chol_rows[home])
            piv = eliminate(piv, scaled_row)
            for c2 in range(c + 1, BLK):
                cols[c2] = eliminate(cols[c2], elts[c2])
        done += chol_rows
        for n in rest:
            upd = groups[n]
            for c in range(BLK):
                upd = upd - mults[n][c] * sublane(piv, c)
            groups[n] = upd
        if between is not None:
            between(b)
    low_inv = jnp.concatenate(done, axis=0)[:, :RANK]
    return dot_tn(low_inv, low_inv, HIGH)


def kernel(x_hbm, b_hbm, c_hbm, lam_ref, a_out, b_out, c_out,
           b_init, c_init, xf, x4, x4t, u_ref, bt, c_own, c_other, cb, a32_ref, at_ref,
           ma_snd, ma_rcv, ga_snd, ga_rcv, mb_part, mb_d2d, mb_sum, mb_rcv, bo_ref,
           g0_snd, g0_rcv, gb_part, gb_snd, gb_rcv, gb_all, mc_snd, mc_rcv, inv_ref,
           in_sem, x_sem, b_ss, b_rs, ma_ss, ma_rs, ga_ss, ga_rs, md_ss, md_rs, my_ss, my_rs,
           ag_ss, ag_rs, g0_ss, g0_rs, gb_ss, gb_rs, mc_ss, mc_rs):
    tube, col, row = lax.axis_index("tube"), lax.axis_index("col"), lax.axis_index("row")

    def peer(d):
        t = 1 - tube if d & 4 else tube
        c = 1 - col if d & 2 else col
        r = 1 - row if d & 1 else row
        return (t, c, r)

    def send(src, dst, ss, rs, d):
        return pltpu.make_async_remote_copy(src_ref=src, dst_ref=dst, send_sem=ss, recv_sem=rs,
                                            device_id=peer(d), device_id_type=MESH)

    def load(n, g):
        rows = pl.ds(g * LOAD_K, LOAD_K)
        return pltpu.make_async_copy(x_hbm.at[rows, :, pl.ds(pl.multiple_of(tile_of(n) * J_TILE, J_TILE), J_TILE)],
                                     xf.at[n, rows], x_sem.at[n, g])

    def tile_of(n):
        if n == 0:
            return row * 2 + tube
        if n == 1:
            return (1 - row) * 2 + tube
        return (3 - n) * 2 + 1 - tube

    small = [pltpu.make_async_copy(src, dst, in_sem.at[n])
             for n, (src, dst) in enumerate(((b_hbm, b_init), (c_hbm, c_init)))]
    for cp in small:
        cp.start()

    def load_start(n):
        for g in range(K_LOC // LOAD_K):
            load(n, g).start(priority=1)

    load_start(0)
    load_start(1)
    barrier = pltpu.get_barrier_semaphore()
    for d in range(1, 8):
        pl.semaphore_signal(barrier, inc=1, device_id=peer(d), device_id_type=MESH)

    k_base = pl.multiple_of(tube * K_LOC, K_LOC)
    k_far = pl.multiple_of((1 - tube) * K_LOC, K_LOC)
    lam = lam_ref[0, 0]
    for cp in small:
        cp.wait()
    for n in range(2, J_TILES):
        load_start(n)
    bt[0, row * 2 + tube] = b_init[...].astype(BF16)

    def turn_c(rows):
        wide = jnp.concatenate([rows, jnp.zeros((K_LOC, RANK), F32)], axis=1)
        return jnp.concatenate([wide, jnp.zeros((LANES - K_LOC, LANES), F32)], axis=0).T[:RANK]

    def spread_c():
        for k in range(K_LOC):
            cb[k] = jnp.broadcast_to(c_own[:, k:k + 1], (RANK, LANES))

    c_own[...] = turn_c(c_init[pl.ds(k_base, K_LOC), :])
    c_other[...] = turn_c(c_init[pl.ds(k_far, K_LOC), :])
    pl.semaphore_wait(barrier, 7)

    def b_send(tile, n, d, ss):
        return send(bt.at[0, tile], bt.at[0, tile], b_ss.at[ss], b_rs.at[n - 1], d)

    own_tile = row * 2 + tube

    @pl.when(row == 0)
    def _():
        b_send(own_tile, 3, 4, 1).start()
        b_send(own_tile, 3, 5, 2).start()

    @pl.when(row == 1)
    def _():
        b_send(own_tile, 2, 4, 1).start()

    b_send(own_tile, 1, 1, 0).start()

    half_lanes = lax.broadcasted_iota(jnp.int32, (RANK // 2, LANES), 1) < RANK

    def gram_dup(turned):
        return dot_nt(turned, jnp.concatenate([turned, turned], axis=0))

    def gram_pack(tiles):
        gram = sum(gram_dup(tile) for tile in tiles)
        return jnp.where(half_lanes, gram[:RANK // 2], gram[RANK // 2:])

    def gram_unpack(packed):
        turned = pltpu.roll(packed, RANK, 1)
        return jnp.concatenate([jnp.where(half_lanes, packed, turned), jnp.where(half_lanes, turned, packed)], axis=0)

    def g0_send(d):
        return send(g0_snd, g0_rcv.at[d - 1], g0_ss.at[d - 1], g0_rs.at[d - 1], d)

    def gb_send(s, d):
        return send(gb_snd, gb_rcv.at[s, d - 1], gb_ss.at[d - 1], gb_rs.at[s, d - 1], d)

    def gram_b_sent(s):
        for d in (1, 2, 3):
            gb_send(s, d).wait_send()

    def gram_b_start(s):
        pl.when(s > 0)(lambda: gram_b_sent(s - 1))
        gb_snd[...] = gb_part[...] + gram_pack([bt[s + 1, row * 2 + 1]])
        for core in range(2):
            n = 1 + (row if core == 0 else 1 - row)
            pltpu.make_async_remote_copy(src_ref=gb_snd, dst_ref=gb_rcv.at[s, n], send_sem=gb_ss.at[n],
                                         recv_sem=gb_rs.at[s, n], device_id=(tube, 1 - col, core),
                                         device_id_type=MESH).start()
        gb_send(s, 1).start()

    def gram_b_finish(s):
        for d in (3, 2, 1):
            gb_send(s, d).wait_recv()
        gb_all[...] = gram_unpack((gb_snd[...] + gb_rcv[s, 0]) + (gb_rcv[s, 1] + gb_rcv[s, 2]))

    lanes_c = lax.broadcasted_iota(jnp.int32, (K_LOC // 2, LANES), 1)

    def u_pass(slot, tiles, first, last, staged=None, slabs=range(K_LOC)):
        packed = jnp.zeros((K_LOC // 2, LANES), F32)
        for k in slabs:
            u_new = jnp.zeros((RANK, I_LOC), F32)
            for jt in tiles:
                if staged is None:
                    x_turn = x4t[jt, k]
                else:
                    x_tile = xf[staged, k].astype(BF16)
                    x4[jt, k] = x_tile
                    x_turn = x_tile.T
                    x4t[jt, k] = x_turn
                u_new = u_new + dot_nn(bt[slot, jt], x_turn)
            if not first:
                u_new = u_ref[k] + u_new
            u_ref[k] = u_new
            if last:
                prod = u_new[:, :I_HALF] * a32_ref[0] + u_new[:, I_HALF:] * a32_ref[1]
                for g in range(RANK // 8):
                    total = jnp.sum(prod[8 * g:8 * g + 8], axis=1, keepdims=True)
                    packed = jnp.where(lanes_c == K_LOC * g + k, total, packed)
        return packed

    g0_snd[...] = gram_pack([bt[0, own_tile]])
    for d in (7, 6, 3, 2, 5, 4, 1):
        g0_send(d).start()
    spread_c()
    for n in range(J_TILES):
        if n > 0:
            b_send(tile_of(n), n, 1, 0).wait_recv()
            if n == 2:
                @pl.when(row == 1)
                def _():
                    b_send(tile_of(2), 2, 1, 2).start()
        step = K_LOC // 2 if n == J_TILES - 1 else K_LOC
        for k in range(0, K_LOC, step):
            for g in range(k // LOAD_K, (k + step) // LOAD_K):
                load(n, g).wait()
            u_pass(0, [tile_of(n)], n == 0, False, staged=n, slabs=range(k, k + step))
    for ss in range(3):
        b_send(own_tile, 1, 1, ss).wait_send()
    for d in range(1, 8):
        g0_send(d).wait()
    here = (g0_snd[...] + g0_rcv[0]) + (g0_rcv[3] + g0_rcv[4])
    there = (g0_rcv[1] + g0_rcv[2]) + (g0_rcv[5] + g0_rcv[6])
    gb_all[...] = gram_unpack(here + there)

    def c_send(s, d):
        return send(mc_snd, mc_rcv.at[s, d - 1], mc_ss.at[d - 1], mc_rs.at[s, d - 1], d)

    def c_solve(packed):
        turned = [packed if g == 0 else pltpu.roll(packed, LANES - K_LOC * g, 1) for g in range(RANK // 8)]
        turned = jnp.concatenate(turned, axis=0)
        lane = lax.broadcasted_iota(jnp.int32, (RANK, LANES), 1)
        return dot_nn(inv_ref[...], jnp.where(lane < K_LOC, turned, 0.0), HIGH)

    def c_sent(s):
        for d in range(1, 8):
            c_send(s, d).wait_send()

    def c_near(s):
        c_own[...] = c_solve((mc_snd[...] + mc_rcv[s, 0]) + (mc_rcv[s, 1] + mc_rcv[s, 2]))

    def c_far(s):
        c_other[...] = c_solve((mc_rcv[s, 3] + mc_rcv[s, 4]) + (mc_rcv[s, 5] + mc_rcv[s, 6]))

    def c_far_wait(s):
        for d in (4, 5, 6, 7):
            c_send(s, d).wait_recv()

    def a_send(s, ch, d):
        n = d // 2 - 1
        return send(ma_snd.at[ch], ma_rcv.at[s, n, ch], ma_ss.at[n, ch], ma_rs.at[s, n, ch], d)

    def a_start(s, spread):
        parts = [jnp.zeros((RANK, I_HALF), F32) for _ in range(A_CHUNKS)]
        for k in range(K_LOC):
            if spread:
                c_col = jnp.broadcast_to(c_own[:, k:k + 1], (RANK, LANES))
                cb[k] = c_col
            else:
                c_col = cb[k]
            for ch in range(A_CHUNKS):
                parts[ch] = parts[ch] + u_ref[k, :, ch * I_HALF:(ch + 1) * I_HALF] * c_col
        for ch in range(A_CHUNKS):
            ma_snd[ch] = parts[ch]
            for d in (6, 4, 2):
                a_send(s, ch, d).start()

    a_start(0, False)

    @pl.loop(0, SWEEPS)
    def _(s):
        @pl.when(s > 0)
        def _():
            c_far_wait(s - 1)
            c_far(s - 1)

        gram_c = gram_dup(c_own[...].astype(BF16)) + gram_dup(c_other[...].astype(BF16))
        inv_a = spd_inverse(gb_all[...] * gram_c, lam)
        def a_solve(ch):
            for d in (2, 4, 6):
                a_send(s, ch, d).wait_recv()
            mtt_a = (ma_snd[ch] + ma_rcv[s, 0, ch]) + (ma_rcv[s, 1, ch] + ma_rcv[s, 2, ch])
            a_turn = dot_nn(inv_a, mtt_a, HIGH)
            a32_ref[ch] = a_turn
            at_ref[ch] = a_turn.astype(BF16)

        def v_tile(jt, ch):
            acc = jnp.zeros((RANK, J_TILE), F32)
            for k in range(K_LOC):
                v_kt = dot_nn(at_ref[ch], x4[jt, k, ch * I_HALF:(ch + 1) * I_HALF, :])
                c_col = cb[k]
                acc = acc + v_kt * jnp.concatenate([c_col, c_col], axis=1)
            return acc

        def d_send(q):
            return send(mb_part.at[(1 - row) * 2 + q], mb_d2d.at[s, q], md_ss.at[q], md_rs.at[s, q], 1)

        def y_send(q):
            return send(mb_sum.at[q], mb_rcv.at[s, q], my_ss.at[q], my_rs.at[s, q], 4)

        def ga_send():
            return send(ga_snd, ga_rcv.at[s], ga_ss, ga_rs.at[s], 1)

        def reduce_cores(q):
            d_send(q).wait_recv()
            mb_sum[q] = mb_part[row * 2 + q] + mb_d2d[s, q]
            y_send(q).start()

        a_solve(0)
        for jt in range(J_TILES):
            mb_part[jt] = v_tile(jt, 0)
        a_solve(1)

        def v_last(jt):
            mb_part[jt] = mb_part[jt] + v_tile(jt, 1)

        v_last(0)

        @pl.when(row == 0)
        def _():
            reduce_cores(0)

        @pl.when(row == 1)
        def _():
            d_send(0).start()

        v_last(2)
        ga_snd[...] = sum(gram_dup(at_ref[ch]) for ch in range(A_CHUNKS))

        @pl.when(row == 0)
        def _():
            d_send(0).start()

        ga_send().start()
        v_last(1)
        v_last(3)

        @pl.when(row == 0)
        def _():
            reduce_cores(1)

        d_send(1).start()

        def late_reduce(b):
            if b == 0:
                @pl.when(row == 1)
                def _():
                    reduce_cores(1)

        @pl.when(row == 1)
        def _():
            reduce_cores(0)

        ga_send().wait_recv()
        gram_a = ga_snd[...] + ga_rcv[s]
        inv_b = spd_inverse(gram_a * gram_c, lam, late_reduce)
        g_copies = []

        def b_solve(q):
            y_send(q).wait_recv()
            b_new = dot_nn(inv_b, mb_sum[q] + mb_rcv[s, q], HIGH)
            bo_ref[q] = b_new
            tile = bt.at[s + 1, row * 2 + q]
            tile[...] = b_new.astype(BF16)
            cp = send(tile, tile, ag_ss.at[q], ag_rs.at[s, q], 1)
            cp.start()
            g_copies.append(cp)

        b_solve(0)
        gb_part[...] = gram_pack([bt[s + 1, row * 2]])
        b_solve(1)
        gram_b_start(s)
        u_pass(s + 1, [row * 2, row * 2 + 1], True, False)
        g_copies[0].wait_recv()
        u_pass(s + 1, [(1 - row) * 2], False, False)
        g_copies[1].wait_recv()
        part_c = u_pass(s + 1, [(1 - row) * 2 + 1], False, True)

        @pl.when(s > 0)
        def _():
            c_sent(s - 1)

        mc_snd[...] = part_c
        for d in (6, 7, 2, 3, 4, 5, 1):
            c_send(s, d).start()
        for ch in range(A_CHUNKS):
            for d in (2, 4, 6):
                a_send(s, ch, d).wait_send()
        ga_send().wait_send()
        for q in range(2):
            d_send(q).wait_send()
            y_send(q).wait_send()
            g_copies[q].wait_send()
        a_rows = a32_ref[col].T
        a_out[...] = jnp.where(tube == 0, a_rows[:I_HALF // 2], a_rows[I_HALF // 2:])
        b_out[...] = bo_ref[tube]
        gram_b_finish(s)
        inv_ref[...] = spd_inverse(gram_a * gb_all[...], lam)
        for d in (1, 2, 3):
            c_send(s, d).wait_recv()

        @pl.when(s < SWEEPS - 1)
        def _():
            c_near(s)
            a_start(s + 1, True)

    c_far_wait(SWEEPS - 1)
    c_near(SWEEPS - 1)
    c_far(SWEEPS - 1)
    c_sent(SWEEPS - 1)
    gram_b_sent(SWEEPS - 1)
    c_out[pl.ds(k_base, K_LOC), :] = c_own[...].T[:K_LOC]
    c_out[pl.ds(k_far, K_LOC), :] = c_other[...].T[:K_LOC]


def emit(a_in, b_in, c_in, a_hbm, b_hbm, c_hbm, sems):
    pairs = ((b_in, b_hbm), (a_in, a_hbm), (c_in, c_hbm))
    copies = [pltpu.make_async_copy(src, dst, sems.at[n]) for n, (src, dst) in enumerate(pairs)]
    for cp in copies:
        cp.start()
    for cp in copies:
        cp.wait()


def solution(mesh):
    def local(x_blk, b_own, c_full, ridge_lam):
        shapes = ((64, RANK), (RANK, 256), (32, RANK))
        operands = (x_blk, b_own.T, c_full)
        operands = [pltpu.with_memory_space_constraint(v, pltpu.HBM) for v in operands]
        dma = pltpu.SemaphoreType.DMA
        vm = pltpu.VMEM
        a_new, b_new, c_new = pl.pallas_call(
            kernel,
            out_shape=tuple(pltpu.VMEM(shape, F32) for shape in shapes),
            in_specs=[pl.BlockSpec(memory_space=pltpu.HBM)] * 3 + [pl.BlockSpec(memory_space=pltpu.SMEM)],
            out_specs=(pl.BlockSpec(memory_space=pltpu.VMEM),) * 3,
            scratch_shapes=[
                vm((RANK, J_TILE), F32),
                vm((2 * K_LOC, RANK), F32),
                vm((J_TILES, K_LOC, I_LOC, J_TILE), F32),
                vm((J_TILES, K_LOC, I_LOC, J_TILE), BF16),
                vm((J_TILES, K_LOC, J_TILE, I_LOC), BF16),
                vm((K_LOC, RANK, I_LOC), F32),
                vm((SWEEPS + 1, J_TILES, RANK, J_TILE), BF16),
                vm((RANK, LANES), F32),
                vm((RANK, LANES), F32),
                vm((K_LOC, RANK, LANES), F32),
                vm((A_CHUNKS, RANK, I_HALF), F32),
                vm((A_CHUNKS, RANK, I_HALF), BF16),
                vm((A_CHUNKS, RANK, I_HALF), F32),
                vm((SWEEPS, 3, A_CHUNKS, RANK, I_HALF), F32),
                vm((RANK, LANES), F32),
                vm((SWEEPS, RANK, LANES), F32),
                vm((J_TILES, RANK, J_TILE), F32),
                vm((SWEEPS, 2, RANK, J_TILE), F32),
                vm((2, RANK, J_TILE), F32),
                vm((SWEEPS, 2, RANK, J_TILE), F32),
                vm((2, RANK, J_TILE), F32),
                vm((RANK // 2, LANES), F32),
                vm((7, RANK // 2, LANES), F32),
                vm((RANK // 2, LANES), F32),
                vm((RANK // 2, LANES), F32),
                vm((SWEEPS, 3, RANK // 2, LANES), F32),
                vm((RANK, LANES), F32),
                vm((K_LOC // 2, LANES), F32),
                vm((SWEEPS, 7, K_LOC // 2, LANES), F32),
                vm((RANK, RANK), F32),
                dma((2,)), dma((J_TILES, K_LOC // LOAD_K)), dma((3,)), dma((3,)),
                dma((3, A_CHUNKS)), dma((SWEEPS, 3, A_CHUNKS)),
                dma, dma((SWEEPS,)),
                dma((2,)), dma((SWEEPS, 2)), dma((2,)), dma((SWEEPS, 2)),
                dma((2,)), dma((SWEEPS, 2)),
                dma((7,)), dma((7,)), dma((3,)), dma((SWEEPS, 3)),
                dma((7,)), dma((SWEEPS, 7)),
            ],
            compiler_params=pltpu.CompilerParams(collective_id=0, has_side_effects=True,
                                                 vmem_limit_bytes=52 * 1024 * 1024),
            name="als_sweeps",
        )(*operands, ridge_lam.reshape(1, 1))
        a_new, b_new, c_new = pl.pallas_call(
            emit,
            out_shape=tuple(jax.ShapeDtypeStruct(shape, F32) for shape in shapes),
            in_specs=[pl.BlockSpec(memory_space=pltpu.VMEM)] * 3,
            out_specs=(pl.BlockSpec(memory_space=pl.ANY),) * 3,
            scratch_shapes=[dma((3,))],
            compiler_params=pltpu.CompilerParams(vmem_limit_bytes=1024 * 1024),
            name="emit_factors",
        )(a_new, b_new, c_new)
        return a_new, b_new.T, c_new

    return jax.shard_map(
        local,
        mesh=mesh,
        in_specs=(P("tube", "row", "col"), P(("col", "row", "tube"), None), P(None, None), P()),
        out_specs=(P(("row", "col", "tube"), None), P(("col", "row", "tube"), None), P(None, None)),
        check_vma=False,
    )
```

```python
import jax
import jax.numpy as jnp
from jax import lax
from jax.experimental import pallas as pl
from jax.experimental.pallas import tpu as pltpu
from jax.sharding import PartitionSpec as P

SWEEPS = 2
RANK = 64
LANES = 128
K_LOC = 16
I_LOC = 256
J_TILE = 256
J_TILES = 4
I_HALF = I_LOC // 2
A_CHUNKS = 2
BLK = 16
SUB = 8
LOAD_K = 4
MESH = pl.DeviceIdType.MESH
HIGH = lax.Precision.HIGHEST
F32 = jnp.float32
BF16 = jnp.bfloat16


def dot_nn(a, b, precision=None):
    return lax.dot_general(a, b, (((1,), (0,)), ((), ())), precision=precision, preferred_element_type=F32)


def dot_nt(a, b, precision=None):
    return lax.dot_general(a, b, (((1,), (1,)), ((), ())), precision=precision, preferred_element_type=F32)


def dot_tn(a, b, precision=None):
    return lax.dot_general(a, b, (((0,), (0,)), ((), ())), precision=precision, preferred_element_type=F32)


def spd_inverse(gram_dup, lam, between=None):
    row_ids = lax.broadcasted_iota(jnp.int32, (RANK, LANES), 0)
    lane_ids = lax.broadcasted_iota(jnp.int32, (RANK, LANES), 1)
    left_eye = jnp.where(lane_ids == row_ids, 1.0, 0.0).astype(F32)
    right_eye = jnp.where(lane_ids == row_ids + RANK, 1.0, 0.0).astype(F32)
    aug = jnp.where(lane_ids < RANK, left_eye, gram_dup + lam * right_eye)
    groups = [aug[n * SUB:(n + 1) * SUB] for n in range(RANK // SUB)]
    sub_ids = lax.broadcasted_iota(jnp.int32, (SUB, LANES), 0)
    per_blk = BLK // SUB

    def lane(group, at):
        return jnp.broadcast_to(group[:, at:at + 1], (SUB, LANES))

    def sublane(parts, c):
        part = parts[c // SUB]
        return jnp.broadcast_to(part[c % SUB:c % SUB + 1, :], (SUB, LANES))

    done = []
    for b in range(RANK // BLK):
        first, start = b * per_blk, RANK + b * BLK
        piv = groups[first:first + per_blk]
        cols = [[lane(part, start + c) for part in piv] for c in range(BLK)]
        rest = range(first + per_blk, RANK // SUB)
        mults = {n: [lane(groups[n], start + c) for c in range(BLK)] for n in rest}
        chol_rows = [jnp.zeros((SUB, LANES), F32) for _ in range(per_blk)]
        diag = sublane(cols[0], 0)
        for c in range(BLK):
            is_row = sub_ids == c % SUB
            home = c // SUB
            root = lax.rsqrt(diag)
            elts = {c2: sublane(cols[c2], c) * root for c2 in range(c + 1, BLK)}
            if c + 1 < BLK:
                diag = sublane(cols[c + 1], c + 1) - (sublane(cols[c], c + 1) * root) * elts[c + 1]
            scaled_col = [part * root for part in cols[c]]
            scaled_row = sublane(piv, c) * root

            def eliminate(parts, elt):
                new = [part - scale * elt for part, scale in zip(parts, scaled_col)]
                new[home] = jnp.where(is_row, elt * root, new[home])
                return new

            chol_rows[home] = jnp.where(is_row, scaled_row, chol_rows[home])
            piv = eliminate(piv, scaled_row)
            for c2 in range(c + 1, BLK):
                cols[c2] = eliminate(cols[c2], elts[c2])
        done += chol_rows
        for n in rest:
            upd = groups[n]
            for c in range(BLK):
                upd = upd - mults[n][c] * sublane(piv, c)
            groups[n] = upd
        if between is not None:
            between(b)
    low_inv = jnp.concatenate(done, axis=0)[:, :RANK]
    return dot_tn(low_inv, low_inv, HIGH)


def kernel(x_hbm, b_hbm, c_hbm, lam_ref, a_out, b_out, c_out,
           b_init, c_init, xf, x4, x4t, u_ref, bt, c_own, c_other, cb, a32_ref, at_ref,
           ma_snd, ma_rcv, ga_snd, ga_rcv, mb_part, mb_d2d, mb_sum, mb_rcv, bo_ref,
           g0_snd, g0_rcv, gb_part, gb_snd, gb_rcv, gb_all, mc_snd, mc_rcv, inv_ref,
           in_sem, x_sem, b_ss, b_rs, ma_ss, ma_rs, ga_ss, ga_rs, md_ss, md_rs, my_ss, my_rs,
           ag_ss, ag_rs, g0_ss, g0_rs, gb_ss, gb_rs, mc_ss, mc_rs):
    tube, col, row = lax.axis_index("tube"), lax.axis_index("col"), lax.axis_index("row")

    def peer(d):
        t = 1 - tube if d & 4 else tube
        c = 1 - col if d & 2 else col
        r = 1 - row if d & 1 else row
        return (t, c, r)

    def send(src, dst, ss, rs, d):
        return pltpu.make_async_remote_copy(src_ref=src, dst_ref=dst, send_sem=ss, recv_sem=rs,
                                            device_id=peer(d), device_id_type=MESH)

    def load(n, g):
        rows = pl.ds(g * LOAD_K, LOAD_K)
        return pltpu.make_async_copy(x_hbm.at[rows, :, pl.ds(pl.multiple_of(tile_of(n) * J_TILE, J_TILE), J_TILE)],
                                     xf.at[n, rows], x_sem.at[n, g])

    def tile_of(n):
        if n == 0:
            return row * 2 + tube
        if n == 1:
            return (1 - row) * 2 + tube
        return (3 - n) * 2 + 1 - tube

    small = [pltpu.make_async_copy(src, dst, in_sem.at[n])
             for n, (src, dst) in enumerate(((b_hbm, b_init), (c_hbm, c_init)))]
    for cp in small:
        cp.start()

    def load_start(n):
        for g in range(K_LOC // LOAD_K):
            load(n, g).start(priority=1)

    load_start(0)
    load_start(1)
    barrier = pltpu.get_barrier_semaphore()
    for d in range(1, 8):
        pl.semaphore_signal(barrier, inc=1, device_id=peer(d), device_id_type=MESH)

    k_base = pl.multiple_of(tube * K_LOC, K_LOC)
    k_far = pl.multiple_of((1 - tube) * K_LOC, K_LOC)
    lam = lam_ref[0, 0]
    for cp in small:
        cp.wait()
    for n in range(2, J_TILES):
        load_start(n)
    bt[0, row * 2 + tube] = b_init[...].astype(BF16)

    def turn_c(rows):
        wide = jnp.concatenate([rows, jnp.zeros((K_LOC, RANK), F32)], axis=1)
        return jnp.concatenate([wide, jnp.zeros((LANES - K_LOC, LANES), F32)], axis=0).T[:RANK]

    def spread_c():
        for k in range(K_LOC):
            cb[k] = jnp.broadcast_to(c_own[:, k:k + 1], (RANK, LANES))

    c_own[...] = turn_c(c_init[pl.ds(k_base, K_LOC), :])
    c_other[...] = turn_c(c_init[pl.ds(k_far, K_LOC), :])
    pl.semaphore_wait(barrier, 7)

    def b_send(tile, n, d, ss):
        return send(bt.at[0, tile], bt.at[0, tile], b_ss.at[ss], b_rs.at[n - 1], d)

    own_tile = row * 2 + tube

    @pl.when(row == 0)
    def _():
        b_send(own_tile, 3, 4, 1).start()
        b_send(own_tile, 3, 5, 2).start()

    @pl.when(row == 1)
    def _():
        b_send(own_tile, 2, 4, 1).start()

    b_send(own_tile, 1, 1, 0).start()

    half_lanes = lax.broadcasted_iota(jnp.int32, (RANK // 2, LANES), 1) < RANK

    def gram_dup(turned):
        return dot_nt(turned, jnp.concatenate([turned, turned], axis=0))

    def gram_pack(tiles):
        gram = sum(gram_dup(tile) for tile in tiles)
        return jnp.where(half_lanes, gram[:RANK // 2], gram[RANK // 2:])

    def gram_unpack(packed):
        turned = pltpu.roll(packed, RANK, 1)
        return jnp.concatenate([jnp.where(half_lanes, packed, turned), jnp.where(half_lanes, turned, packed)], axis=0)

    def g0_send(d):
        return send(g0_snd, g0_rcv.at[d - 1], g0_ss.at[d - 1], g0_rs.at[d - 1], d)

    def gb_send(s, d):
        return send(gb_snd, gb_rcv.at[s, d - 1], gb_ss.at[d - 1], gb_rs.at[s, d - 1], d)

    def gram_b_sent(s):
        for d in (1, 2, 3):
            gb_send(s, d).wait_send()

    def gram_b_start(s):
        pl.when(s > 0)(lambda: gram_b_sent(s - 1))
        gb_snd[...] = gb_part[...] + gram_pack([bt[s + 1, row * 2 + 1]])
        for core in range(2):
            n = 1 + (row if core == 0 else 1 - row)
            pltpu.make_async_remote_copy(src_ref=gb_snd, dst_ref=gb_rcv.at[s, n], send_sem=gb_ss.at[n],
                                         recv_sem=gb_rs.at[s, n], device_id=(tube, 1 - col, core),
                                         device_id_type=MESH).start()
        gb_send(s, 1).start()

    def gram_b_finish(s):
        for d in (3, 2, 1):
            gb_send(s, d).wait_recv()
        gb_all[...] = gram_unpack((gb_snd[...] + gb_rcv[s, 0]) + (gb_rcv[s, 1] + gb_rcv[s, 2]))

    lanes_c = lax.broadcasted_iota(jnp.int32, (K_LOC // 2, LANES), 1)

    def u_pass(slot, tiles, first, last, staged=None, slabs=range(K_LOC)):
        packed = jnp.zeros((K_LOC // 2, LANES), F32)
        for k in slabs:
            u_new = jnp.zeros((RANK, I_LOC), F32)
            for jt in tiles:
                if staged is None:
                    x_turn = x4t[jt, k]
                else:
                    x_tile = xf[staged, k].astype(BF16)
                    x4[jt, k] = x_tile
                    x_turn = x_tile.T
                    x4t[jt, k] = x_turn
                u_new = u_new + dot_nn(bt[slot, jt], x_turn)
            if not first:
                u_new = u_ref[k] + u_new
            u_ref[k] = u_new
            if last:
                prod = u_new[:, :I_HALF] * a32_ref[0] + u_new[:, I_HALF:] * a32_ref[1]
                for g in range(RANK // 8):
                    total = jnp.sum(prod[8 * g:8 * g + 8], axis=1, keepdims=True)
                    packed = jnp.where(lanes_c == K_LOC * g + k, total, packed)
        return packed

    g0_snd[...] = gram_pack([bt[0, own_tile]])
    for d in (7, 6, 3, 2, 5, 4, 1):
        g0_send(d).start()
    spread_c()
    for n in range(J_TILES):
        if n > 0:
            b_send(tile_of(n), n, 1, 0).wait_recv()
            if n == 2:
                @pl.when(row == 1)
                def _():
                    b_send(tile_of(2), 2, 1, 2).start()
        step = K_LOC // 2 if n == J_TILES - 1 else K_LOC
        for k in range(0, K_LOC, step):
            for g in range(k // LOAD_K, (k + step) // LOAD_K):
                load(n, g).wait()
            u_pass(0, [tile_of(n)], n == 0, False, staged=n, slabs=range(k, k + step))
    for ss in range(3):
        b_send(own_tile, 1, 1, ss).wait_send()
    for d in range(1, 8):
        g0_send(d).wait()
    here = (g0_snd[...] + g0_rcv[0]) + (g0_rcv[3] + g0_rcv[4])
    there = (g0_rcv[1] + g0_rcv[2]) + (g0_rcv[5] + g0_rcv[6])
    gb_all[...] = gram_unpack(here + there)

    def c_send(s, d):
        return send(mc_snd, mc_rcv.at[s, d - 1], mc_ss.at[d - 1], mc_rs.at[s, d - 1], d)

    def c_solve(packed):
        turned = [packed if g == 0 else pltpu.roll(packed, LANES - K_LOC * g, 1) for g in range(RANK // 8)]
        turned = jnp.concatenate(turned, axis=0)
        lane = lax.broadcasted_iota(jnp.int32, (RANK, LANES), 1)
        return dot_nn(inv_ref[...], jnp.where(lane < K_LOC, turned, 0.0), HIGH)

    def c_sent(s):
        for d in range(1, 8):
            c_send(s, d).wait_send()

    def c_near(s):
        c_own[...] = c_solve((mc_snd[...] + mc_rcv[s, 0]) + (mc_rcv[s, 1] + mc_rcv[s, 2]))

    def c_far(s):
        c_other[...] = c_solve((mc_rcv[s, 3] + mc_rcv[s, 4]) + (mc_rcv[s, 5] + mc_rcv[s, 6]))

    def c_far_wait(s):
        for d in (4, 5, 6, 7):
            c_send(s, d).wait_recv()

    def a_send(s, ch, d):
        n = d // 2 - 1
        return send(ma_snd.at[ch], ma_rcv.at[s, n, ch], ma_ss.at[n, ch], ma_rs.at[s, n, ch], d)

    def a_start(s, spread):
        parts = [jnp.zeros((RANK, I_HALF), F32) for _ in range(A_CHUNKS)]
        for k in range(K_LOC):
            if spread:
                c_col = jnp.broadcast_to(c_own[:, k:k + 1], (RANK, LANES))
                cb[k] = c_col
            else:
                c_col = cb[k]
            for ch in range(A_CHUNKS):
                parts[ch] = parts[ch] + u_ref[k, :, ch * I_HALF:(ch + 1) * I_HALF] * c_col
        for ch in range(A_CHUNKS):
            ma_snd[ch] = parts[ch]
            for d in (6, 4, 2):
                a_send(s, ch, d).start()

    a_start(0, False)

    @pl.loop(0, SWEEPS)
    def _(s):
        @pl.when(s > 0)
        def _():
            c_far_wait(s - 1)
            c_far(s - 1)

        gram_c = gram_dup(c_own[...].astype(BF16)) + gram_dup(c_other[...].astype(BF16))
        inv_a = spd_inverse(gb_all[...] * gram_c, lam)
        def a_solve(ch):
            for d in (2, 4, 6):
                a_send(s, ch, d).wait_recv()
            mtt_a = (ma_snd[ch] + ma_rcv[s, 0, ch]) + (ma_rcv[s, 1, ch] + ma_rcv[s, 2, ch])
            a_turn = dot_nn(inv_a, mtt_a, HIGH)
            a32_ref[ch] = a_turn
            at_ref[ch] = a_turn.astype(BF16)

        def v_tile(jt, ch):
            acc = jnp.zeros((RANK, J_TILE), F32)
            for k in range(K_LOC):
                v_kt = dot_nn(at_ref[ch], x4[jt, k, ch * I_HALF:(ch + 1) * I_HALF, :])
                c_col = cb[k]
                acc = acc + v_kt * jnp.concatenate([c_col, c_col], axis=1)
            return acc

        def d_send(q):
            return send(mb_part.at[(1 - row) * 2 + q], mb_d2d.at[s, q], md_ss.at[q], md_rs.at[s, q], 1)

        def y_send(q):
            return send(mb_sum.at[q], mb_rcv.at[s, q], my_ss.at[q], my_rs.at[s, q], 4)

        def ga_send():
            return send(ga_snd, ga_rcv.at[s], ga_ss, ga_rs.at[s], 1)

        def reduce_cores(q):
            d_send(q).wait_recv()
            mb_sum[q] = mb_part[row * 2 + q] + mb_d2d[s, q]
            y_send(q).start()

        a_solve(0)
        for jt in range(J_TILES):
            mb_part[jt] = v_tile(jt, 0)
        a_solve(1)

        def v_last(jt):
            mb_part[jt] = mb_part[jt] + v_tile(jt, 1)

        v_last(0)

        @pl.when(row == 0)
        def _():
            reduce_cores(0)

        @pl.when(row == 1)
        def _():
            d_send(0).start()

        v_last(2)
        ga_snd[...] = sum(gram_dup(at_ref[ch]) for ch in range(A_CHUNKS))

        @pl.when(row == 0)
        def _():
            d_send(0).start()

        ga_send().start()
        v_last(1)

        @pl.when(row == 0)
        def _():
            reduce_cores(1)

        @pl.when(row == 1)
        def _():
            d_send(1).start()

        v_last(3)

        @pl.when(row == 0)
        def _():
            d_send(1).start()

        def late_reduce(b):
            if b == 0:
                @pl.when(row == 1)
                def _():
                    reduce_cores(1)

        @pl.when(row == 1)
        def _():
            reduce_cores(0)

        ga_send().wait_recv()
        gram_a = ga_snd[...] + ga_rcv[s]
        inv_b = spd_inverse(gram_a * gram_c, lam, late_reduce)
        g_copies = []

        def b_solve(q):
            y_send(q).wait_recv()
            b_new = dot_nn(inv_b, mb_sum[q] + mb_rcv[s, q], HIGH)
            bo_ref[q] = b_new
            tile = bt.at[s + 1, row * 2 + q]
            tile[...] = b_new.astype(BF16)
            cp = send(tile, tile, ag_ss.at[q], ag_rs.at[s, q], 1)
            cp.start()
            g_copies.append(cp)

        b_solve(0)
        gb_part[...] = gram_pack([bt[s + 1, row * 2]])
        b_solve(1)
        gram_b_start(s)
        u_pass(s + 1, [row * 2, row * 2 + 1], True, False)
        g_copies[0].wait_recv()
        u_pass(s + 1, [(1 - row) * 2], False, False)
        g_copies[1].wait_recv()
        part_c = u_pass(s + 1, [(1 - row) * 2 + 1], False, True)

        @pl.when(s > 0)
        def _():
            c_sent(s - 1)

        mc_snd[...] = part_c
        for d in (6, 7, 2, 3, 4, 5, 1):
            c_send(s, d).start()
        for ch in range(A_CHUNKS):
            for d in (2, 4, 6):
                a_send(s, ch, d).wait_send()
        ga_send().wait_send()
        for q in range(2):
            d_send(q).wait_send()
            y_send(q).wait_send()
            g_copies[q].wait_send()
        a_rows = a32_ref[col].T
        a_out[...] = jnp.where(tube == 0, a_rows[:I_HALF // 2], a_rows[I_HALF // 2:])
        b_out[...] = bo_ref[tube]
        gram_b_finish(s)
        inv_ref[...] = spd_inverse(gram_a * gb_all[...], lam)
        for d in (1, 2, 3):
            c_send(s, d).wait_recv()

        @pl.when(s < SWEEPS - 1)
        def _():
            c_near(s)
            a_start(s + 1, True)

    c_far_wait(SWEEPS - 1)
    c_near(SWEEPS - 1)
    c_far(SWEEPS - 1)
    c_sent(SWEEPS - 1)
    gram_b_sent(SWEEPS - 1)
    c_out[pl.ds(k_base, K_LOC), :] = c_own[...].T[:K_LOC]
    c_out[pl.ds(k_far, K_LOC), :] = c_other[...].T[:K_LOC]


def emit(a_in, b_in, c_in, a_hbm, b_hbm, c_hbm, sems):
    pairs = ((b_in, b_hbm), (a_in, a_hbm), (c_in, c_hbm))
    copies = [pltpu.make_async_copy(src, dst, sems.at[n]) for n, (src, dst) in enumerate(pairs)]
    for cp in copies:
        cp.start()
    for cp in copies:
        cp.wait()


def solution(mesh):
    def local(x_blk, b_own, c_full, ridge_lam):
        shapes = ((64, RANK), (RANK, 256), (32, RANK))
        operands = (x_blk, b_own.T, c_full)
        operands = [pltpu.with_memory_space_constraint(v, pltpu.HBM) for v in operands]
        dma = pltpu.SemaphoreType.DMA
        vm = pltpu.VMEM
        a_new, b_new, c_new = pl.pallas_call(
            kernel,
            out_shape=tuple(pltpu.VMEM(shape, F32) for shape in shapes),
            in_specs=[pl.BlockSpec(memory_space=pltpu.HBM)] * 3 + [pl.BlockSpec(memory_space=pltpu.SMEM)],
            out_specs=(pl.BlockSpec(memory_space=pltpu.VMEM),) * 3,
            scratch_shapes=[
                vm((RANK, J_TILE), F32),
                vm((2 * K_LOC, RANK), F32),
                vm((J_TILES, K_LOC, I_LOC, J_TILE), F32),
                vm((J_TILES, K_LOC, I_LOC, J_TILE), BF16),
                vm((J_TILES, K_LOC, J_TILE, I_LOC), BF16),
                vm((K_LOC, RANK, I_LOC), F32),
                vm((SWEEPS + 1, J_TILES, RANK, J_TILE), BF16),
                vm((RANK, LANES), F32),
                vm((RANK, LANES), F32),
                vm((K_LOC, RANK, LANES), F32),
                vm((A_CHUNKS, RANK, I_HALF), F32),
                vm((A_CHUNKS, RANK, I_HALF), BF16),
                vm((A_CHUNKS, RANK, I_HALF), F32),
                vm((SWEEPS, 3, A_CHUNKS, RANK, I_HALF), F32),
                vm((RANK, LANES), F32),
                vm((SWEEPS, RANK, LANES), F32),
                vm((J_TILES, RANK, J_TILE), F32),
                vm((SWEEPS, 2, RANK, J_TILE), F32),
                vm((2, RANK, J_TILE), F32),
                vm((SWEEPS, 2, RANK, J_TILE), F32),
                vm((2, RANK, J_TILE), F32),
                vm((RANK // 2, LANES), F32),
                vm((7, RANK // 2, LANES), F32),
                vm((RANK // 2, LANES), F32),
                vm((RANK // 2, LANES), F32),
                vm((SWEEPS, 3, RANK // 2, LANES), F32),
                vm((RANK, LANES), F32),
                vm((K_LOC // 2, LANES), F32),
                vm((SWEEPS, 7, K_LOC // 2, LANES), F32),
                vm((RANK, RANK), F32),
                dma((2,)), dma((J_TILES, K_LOC // LOAD_K)), dma((3,)), dma((3,)),
                dma((3, A_CHUNKS)), dma((SWEEPS, 3, A_CHUNKS)),
                dma, dma((SWEEPS,)),
                dma((2,)), dma((SWEEPS, 2)), dma((2,)), dma((SWEEPS, 2)),
                dma((2,)), dma((SWEEPS, 2)),
                dma((7,)), dma((7,)), dma((3,)), dma((SWEEPS, 3)),
                dma((7,)), dma((SWEEPS, 7)),
            ],
            compiler_params=pltpu.CompilerParams(collective_id=0, has_side_effects=True,
                                                 vmem_limit_bytes=52 * 1024 * 1024),
            name="als_sweeps",
        )(*operands, ridge_lam.reshape(1, 1))
        a_new, b_new, c_new = pl.pallas_call(
            emit,
            out_shape=tuple(jax.ShapeDtypeStruct(shape, F32) for shape in shapes),
            in_specs=[pl.BlockSpec(memory_space=pltpu.VMEM)] * 3,
            out_specs=(pl.BlockSpec(memory_space=pl.ANY),) * 3,
            scratch_shapes=[dma((3,))],
            compiler_params=pltpu.CompilerParams(vmem_limit_bytes=1024 * 1024),
            name="emit_factors",
        )(a_new, b_new, c_new)
        return a_new, b_new.T, c_new

    return jax.shard_map(
        local,
        mesh=mesh,
        in_specs=(P("tube", "row", "col"), P(("col", "row", "tube"), None), P(None, None), P()),
        out_specs=(P(("row", "col", "tube"), None), P(("col", "row", "tube"), None), P(None, None)),
        check_vma=False,
    )
```

```python
import jax
import jax.numpy as jnp
from jax import lax
from jax.experimental import pallas as pl
from jax.experimental.pallas import tpu as pltpu
from jax.sharding import PartitionSpec as P

SWEEPS = 2
RANK = 64
LANES = 128
K_LOC = 16
I_LOC = 256
J_TILE = 256
J_TILES = 4
I_HALF = I_LOC // 2
A_CHUNKS = 2
BLK = 16
SUB = 8
LOAD_K = 4
MESH = pl.DeviceIdType.MESH
HIGH = lax.Precision.HIGHEST
F32 = jnp.float32
BF16 = jnp.bfloat16


def dot_nn(a, b, precision=None):
    return lax.dot_general(a, b, (((1,), (0,)), ((), ())), precision=precision, preferred_element_type=F32)


def dot_nt(a, b, precision=None):
    return lax.dot_general(a, b, (((1,), (1,)), ((), ())), precision=precision, preferred_element_type=F32)


def dot_tn(a, b, precision=None):
    return lax.dot_general(a, b, (((0,), (0,)), ((), ())), precision=precision, preferred_element_type=F32)


def spd_inverse(gram_dup, lam, between=None):
    row_ids = lax.broadcasted_iota(jnp.int32, (RANK, LANES), 0)
    lane_ids = lax.broadcasted_iota(jnp.int32, (RANK, LANES), 1)
    left_eye = jnp.where(lane_ids == row_ids, 1.0, 0.0).astype(F32)
    right_eye = jnp.where(lane_ids == row_ids + RANK, 1.0, 0.0).astype(F32)
    aug = jnp.where(lane_ids < RANK, left_eye, gram_dup + lam * right_eye)
    groups = [aug[n * SUB:(n + 1) * SUB] for n in range(RANK // SUB)]
    sub_ids = lax.broadcasted_iota(jnp.int32, (SUB, LANES), 0)
    per_blk = BLK // SUB

    def lane(group, at):
        return jnp.broadcast_to(group[:, at:at + 1], (SUB, LANES))

    def sublane(parts, c):
        part = parts[c // SUB]
        return jnp.broadcast_to(part[c % SUB:c % SUB + 1, :], (SUB, LANES))

    done = []
    for b in range(RANK // BLK):
        first, start = b * per_blk, RANK + b * BLK
        piv = groups[first:first + per_blk]
        cols = [[lane(part, start + c) for part in piv] for c in range(BLK)]
        rest = range(first + per_blk, RANK // SUB)
        mults = {n: [lane(groups[n], start + c) for c in range(BLK)] for n in rest}
        chol_rows = [jnp.zeros((SUB, LANES), F32) for _ in range(per_blk)]
        diag = sublane(cols[0], 0)
        for c in range(BLK):
            is_row = sub_ids == c % SUB
            home = c // SUB
            root = lax.rsqrt(diag)
            elts = {c2: sublane(cols[c2], c) * root for c2 in range(c + 1, BLK)}
            if c + 1 < BLK:
                diag = sublane(cols[c + 1], c + 1) - (sublane(cols[c], c + 1) * root) * elts[c + 1]
            scaled_col = [part * root for part in cols[c]]
            scaled_row = sublane(piv, c) * root

            def eliminate(parts, elt):
                new = [part - scale * elt for part, scale in zip(parts, scaled_col)]
                new[home] = jnp.where(is_row, elt * root, new[home])
                return new

            chol_rows[home] = jnp.where(is_row, scaled_row, chol_rows[home])
            piv = eliminate(piv, scaled_row)
            for c2 in range(c + 1, BLK):
                cols[c2] = eliminate(cols[c2], elts[c2])
        done += chol_rows
        for n in rest:
            upd = groups[n]
            for c in range(BLK):
                upd = upd - mults[n][c] * sublane(piv, c)
            groups[n] = upd
        if between is not None:
            between(b)
    low_inv = jnp.concatenate(done, axis=0)[:, :RANK]
    return dot_tn(low_inv, low_inv, HIGH)


def kernel(x_hbm, b_hbm, c_hbm, lam_ref, a_out, b_out, c_out,
           b_init, c_init, xf, x4, x4t, u_ref, bt, c_own, c_other, cb, a32_ref, at_ref,
           ma_snd, ma_rcv, ga_snd, ga_rcv, mb_part, mb_d2d, mb_sum, mb_rcv, bo_ref,
           g0_snd, g0_rcv, gb_part, gb_snd, gb_rcv, gb_all, mc_snd, mc_rcv, inv_ref,
           in_sem, x_sem, b_ss, b_rs, ma_ss, ma_rs, ga_ss, ga_rs, md_ss, md_rs, my_ss, my_rs,
           ag_ss, ag_rs, g0_ss, g0_rs, gb_ss, gb_rs, mc_ss, mc_rs):
    tube, col, row = lax.axis_index("tube"), lax.axis_index("col"), lax.axis_index("row")

    def peer(d):
        t = 1 - tube if d & 4 else tube
        c = 1 - col if d & 2 else col
        r = 1 - row if d & 1 else row
        return (t, c, r)

    def send(src, dst, ss, rs, d):
        return pltpu.make_async_remote_copy(src_ref=src, dst_ref=dst, send_sem=ss, recv_sem=rs,
                                            device_id=peer(d), device_id_type=MESH)

    def load(n, g):
        rows = pl.ds(g * LOAD_K, LOAD_K)
        return pltpu.make_async_copy(x_hbm.at[rows, :, pl.ds(pl.multiple_of(tile_of(n) * J_TILE, J_TILE), J_TILE)],
                                     xf.at[n, rows], x_sem.at[n, g])

    def tile_of(n):
        if n == 0:
            return row * 2 + tube
        if n == 1:
            return (1 - row) * 2 + tube
        return (3 - n) * 2 + 1 - tube

    small = [pltpu.make_async_copy(src, dst, in_sem.at[n])
             for n, (src, dst) in enumerate(((b_hbm, b_init), (c_hbm, c_init)))]
    for cp in small:
        cp.start()

    def load_start(n):
        for g in range(K_LOC // LOAD_K):
            load(n, g).start(priority=1)

    load_start(0)
    load_start(1)
    barrier = pltpu.get_barrier_semaphore()
    for d in range(1, 8):
        pl.semaphore_signal(barrier, inc=1, device_id=peer(d), device_id_type=MESH)

    k_base = pl.multiple_of(tube * K_LOC, K_LOC)
    k_far = pl.multiple_of((1 - tube) * K_LOC, K_LOC)
    lam = lam_ref[0, 0]
    for cp in small:
        cp.wait()
    for n in range(2, J_TILES):
        load_start(n)
    bt[0, row * 2 + tube] = b_init[...].astype(BF16)

    def turn_c(rows):
        wide = jnp.concatenate([rows, jnp.zeros((K_LOC, RANK), F32)], axis=1)
        return jnp.concatenate([wide, jnp.zeros((LANES - K_LOC, LANES), F32)], axis=0).T[:RANK]

    def spread_c():
        for k in range(K_LOC):
            cb[k] = jnp.broadcast_to(c_own[:, k:k + 1], (RANK, LANES))

    c_own[...] = turn_c(c_init[pl.ds(k_base, K_LOC), :])
    c_other[...] = turn_c(c_init[pl.ds(k_far, K_LOC), :])
    pl.semaphore_wait(barrier, 7)

    def b_send(tile, n, d, ss):
        return send(bt.at[0, tile], bt.at[0, tile], b_ss.at[ss], b_rs.at[n - 1], d)

    own_tile = row * 2 + tube

    @pl.when(row == 0)
    def _():
        b_send(own_tile, 3, 4, 1).start()
        b_send(own_tile, 3, 5, 2).start()

    @pl.when(row == 1)
    def _():
        b_send(own_tile, 2, 4, 1).start()

    b_send(own_tile, 1, 1, 0).start()

    half_lanes = lax.broadcasted_iota(jnp.int32, (RANK // 2, LANES), 1) < RANK

    def gram_dup(turned):
        return dot_nt(turned, jnp.concatenate([turned, turned], axis=0))

    def gram_pack(tiles):
        gram = sum(gram_dup(tile) for tile in tiles)
        return jnp.where(half_lanes, gram[:RANK // 2], gram[RANK // 2:])

    def gram_unpack(packed):
        turned = pltpu.roll(packed, RANK, 1)
        return jnp.concatenate([jnp.where(half_lanes, packed, turned), jnp.where(half_lanes, turned, packed)], axis=0)

    def g0_send(d):
        return send(g0_snd, g0_rcv.at[d - 1], g0_ss.at[d - 1], g0_rs.at[d - 1], d)

    def gb_send(s, d):
        return send(gb_snd, gb_rcv.at[s, d - 1], gb_ss.at[d - 1], gb_rs.at[s, d - 1], d)

    def gram_b_sent(s):
        for d in (1, 2, 3):
            gb_send(s, d).wait_send()

    def gram_b_start(s):
        pl.when(s > 0)(lambda: gram_b_sent(s - 1))
        gb_snd[...] = gb_part[...] + gram_pack([bt[s + 1, row * 2 + 1]])
        for core in range(2):
            n = 1 + (row if core == 0 else 1 - row)
            pltpu.make_async_remote_copy(src_ref=gb_snd, dst_ref=gb_rcv.at[s, n], send_sem=gb_ss.at[n],
                                         recv_sem=gb_rs.at[s, n], device_id=(tube, 1 - col, core),
                                         device_id_type=MESH).start()
        gb_send(s, 1).start()

    def gram_b_finish(s):
        for d in (3, 2, 1):
            gb_send(s, d).wait_recv()
        gb_all[...] = gram_unpack((gb_snd[...] + gb_rcv[s, 0]) + (gb_rcv[s, 1] + gb_rcv[s, 2]))

    lanes_c = lax.broadcasted_iota(jnp.int32, (K_LOC // 2, LANES), 1)

    def u_pass(slot, tiles, first, last, staged=None, slabs=range(K_LOC)):
        packed = jnp.zeros((K_LOC // 2, LANES), F32)
        for k in slabs:
            u_new = jnp.zeros((RANK, I_LOC), F32)
            for jt in tiles:
                if staged is None:
                    x_turn = x4t[jt, k]
                else:
                    x_tile = xf[staged, k].astype(BF16)
                    x4[jt, k] = x_tile
                    x_turn = x_tile.T
                    x4t[jt, k] = x_turn
                u_new = u_new + dot_nn(bt[slot, jt], x_turn)
            if not first:
                u_new = u_ref[k] + u_new
            u_ref[k] = u_new
            if last:
                prod = u_new[:, :I_HALF] * a32_ref[0] + u_new[:, I_HALF:] * a32_ref[1]
                for g in range(RANK // 8):
                    total = jnp.sum(prod[8 * g:8 * g + 8], axis=1, keepdims=True)
                    packed = jnp.where(lanes_c == K_LOC * g + k, total, packed)
        return packed

    g0_snd[...] = gram_pack([bt[0, own_tile]])
    for d in (7, 6, 3, 2, 5, 4, 1):
        g0_send(d).start()
    spread_c()
    for n in range(J_TILES):
        if n > 0:
            b_send(tile_of(n), n, 1, 0).wait_recv()
            if n == 2:
                @pl.when(row == 1)
                def _():
                    b_send(tile_of(2), 2, 1, 2).start()
        step = K_LOC // 2 if n == J_TILES - 1 else K_LOC
        for k in range(0, K_LOC, step):
            for g in range(k // LOAD_K, (k + step) // LOAD_K):
                load(n, g).wait()
            u_pass(0, [tile_of(n)], n == 0, False, staged=n, slabs=range(k, k + step))
    for ss in range(3):
        b_send(own_tile, 1, 1, ss).wait_send()
    for d in range(1, 8):
        g0_send(d).wait()
    here = (g0_snd[...] + g0_rcv[0]) + (g0_rcv[3] + g0_rcv[4])
    there = (g0_rcv[1] + g0_rcv[2]) + (g0_rcv[5] + g0_rcv[6])
    gb_all[...] = gram_unpack(here + there)

    def c_send(s, d):
        return send(mc_snd, mc_rcv.at[s, d - 1], mc_ss.at[d - 1], mc_rs.at[s, d - 1], d)

    def c_solve(packed):
        turned = [packed if g == 0 else pltpu.roll(packed, LANES - K_LOC * g, 1) for g in range(RANK // 8)]
        turned = jnp.concatenate(turned, axis=0)
        lane = lax.broadcasted_iota(jnp.int32, (RANK, LANES), 1)
        return dot_nn(inv_ref[...], jnp.where(lane < K_LOC, turned, 0.0), HIGH)

    def c_sent(s):
        for d in range(1, 8):
            c_send(s, d).wait_send()

    def c_near(s):
        c_own[...] = c_solve((mc_snd[...] + mc_rcv[s, 0]) + (mc_rcv[s, 1] + mc_rcv[s, 2]))

    def c_far(s):
        c_other[...] = c_solve((mc_rcv[s, 3] + mc_rcv[s, 4]) + (mc_rcv[s, 5] + mc_rcv[s, 6]))

    def c_far_wait(s):
        for d in (4, 5, 6, 7):
            c_send(s, d).wait_recv()

    def a_send(s, ch, d):
        n = d // 2 - 1
        return send(ma_snd.at[ch], ma_rcv.at[s, n, ch], ma_ss.at[n, ch], ma_rs.at[s, n, ch], d)

    def a_start(s, spread):
        parts = [jnp.zeros((RANK, I_HALF), F32) for _ in range(A_CHUNKS)]
        for k in range(K_LOC):
            if spread:
                c_col = jnp.broadcast_to(c_own[:, k:k + 1], (RANK, LANES))
                cb[k] = c_col
            else:
                c_col = cb[k]
            for ch in range(A_CHUNKS):
                parts[ch] = parts[ch] + u_ref[k, :, ch * I_HALF:(ch + 1) * I_HALF] * c_col
        for ch in range(A_CHUNKS):
            ma_snd[ch] = parts[ch]
            for d in (6, 4, 2):
                a_send(s, ch, d).start()

    a_start(0, False)

    @pl.loop(0, SWEEPS)
    def _(s):
        @pl.when(s > 0)
        def _():
            c_far_wait(s - 1)
            c_far(s - 1)

        gram_c = gram_dup(c_own[...].astype(BF16)) + gram_dup(c_other[...].astype(BF16))
        inv_a = spd_inverse(gb_all[...] * gram_c, lam)
        def a_solve(ch):
            for d in (2, 4, 6):
                a_send(s, ch, d).wait_recv()
            mtt_a = (ma_snd[ch] + ma_rcv[s, 0, ch]) + (ma_rcv[s, 1, ch] + ma_rcv[s, 2, ch])
            a_turn = dot_nn(inv_a, mtt_a, HIGH)
            a32_ref[ch] = a_turn
            at_ref[ch] = a_turn.astype(BF16)

        def v_tile(jt, ch):
            acc = jnp.zeros((RANK, J_TILE), F32)
            for k in range(K_LOC):
                v_kt = dot_nn(at_ref[ch], x4[jt, k, ch * I_HALF:(ch + 1) * I_HALF, :])
                c_col = cb[k]
                acc = acc + v_kt * jnp.concatenate([c_col, c_col], axis=1)
            return acc

        def d_send(q):
            return send(mb_part.at[(1 - row) * 2 + q], mb_d2d.at[s, q], md_ss.at[q], md_rs.at[s, q], 1)

        def y_send(q):
            return send(mb_sum.at[q], mb_rcv.at[s, q], my_ss.at[q], my_rs.at[s, q], 4)

        def ga_send():
            return send(ga_snd, ga_rcv.at[s], ga_ss, ga_rs.at[s], 1)

        def reduce_cores(q):
            d_send(q).wait_recv()
            mb_sum[q] = mb_part[row * 2 + q] + mb_d2d[s, q]
            y_send(q).start()

        a_solve(0)
        for jt in range(J_TILES):
            mb_part[jt] = v_tile(jt, 0)
        a_solve(1)

        def v_last(jt):
            mb_part[jt] = mb_part[jt] + v_tile(jt, 1)

        v_last(0)

        @pl.when(row == 0)
        def _():
            reduce_cores(0)

        @pl.when(row == 1)
        def _():
            d_send(0).start()

        v_last(1)
        ga_snd[...] = sum(gram_dup(at_ref[ch]) for ch in range(A_CHUNKS))

        @pl.when(row == 0)
        def _():
            reduce_cores(1)

        @pl.when(row == 1)
        def _():
            d_send(1).start()

        ga_send().start()
        v_last(2)

        @pl.when(row == 0)
        def _():
            d_send(0).start()

        v_last(3)

        @pl.when(row == 0)
        def _():
            d_send(1).start()

        def late_reduce(b):
            if b == 0:
                @pl.when(row == 1)
                def _():
                    reduce_cores(1)

        @pl.when(row == 1)
        def _():
            reduce_cores(0)

        ga_send().wait_recv()
        gram_a = ga_snd[...] + ga_rcv[s]
        inv_b = spd_inverse(gram_a * gram_c, lam, late_reduce)
        g_copies = []

        def b_solve(q):
            y_send(q).wait_recv()
            b_new = dot_nn(inv_b, mb_sum[q] + mb_rcv[s, q], HIGH)
            bo_ref[q] = b_new
            tile = bt.at[s + 1, row * 2 + q]
            tile[...] = b_new.astype(BF16)
            cp = send(tile, tile, ag_ss.at[q], ag_rs.at[s, q], 1)
            cp.start()
            g_copies.append(cp)

        b_solve(0)
        gb_part[...] = gram_pack([bt[s + 1, row * 2]])
        b_solve(1)
        gram_b_start(s)
        u_pass(s + 1, [row * 2, row * 2 + 1], True, False)
        g_copies[0].wait_recv()
        u_pass(s + 1, [(1 - row) * 2], False, False)
        g_copies[1].wait_recv()
        part_c = u_pass(s + 1, [(1 - row) * 2 + 1], False, True)

        @pl.when(s > 0)
        def _():
            c_sent(s - 1)

        mc_snd[...] = part_c
        for d in (6, 7, 2, 3, 4, 5, 1):
            c_send(s, d).start()
        for ch in range(A_CHUNKS):
            for d in (2, 4, 6):
                a_send(s, ch, d).wait_send()
        ga_send().wait_send()
        for q in range(2):
            d_send(q).wait_send()
            y_send(q).wait_send()
            g_copies[q].wait_send()
        a_rows = a32_ref[col].T
        a_out[...] = jnp.where(tube == 0, a_rows[:I_HALF // 2], a_rows[I_HALF // 2:])
        b_out[...] = bo_ref[tube]
        gram_b_finish(s)
        inv_ref[...] = spd_inverse(gram_a * gb_all[...], lam)
        for d in (1, 2, 3):
            c_send(s, d).wait_recv()

        @pl.when(s < SWEEPS - 1)
        def _():
            c_near(s)
            a_start(s + 1, True)

    c_far_wait(SWEEPS - 1)
    c_near(SWEEPS - 1)
    c_far(SWEEPS - 1)
    c_sent(SWEEPS - 1)
    gram_b_sent(SWEEPS - 1)
    c_out[pl.ds(k_base, K_LOC), :] = c_own[...].T[:K_LOC]
    c_out[pl.ds(k_far, K_LOC), :] = c_other[...].T[:K_LOC]


def emit(a_in, b_in, c_in, a_hbm, b_hbm, c_hbm, sems):
    pairs = ((b_in, b_hbm), (a_in, a_hbm), (c_in, c_hbm))
    copies = [pltpu.make_async_copy(src, dst, sems.at[n]) for n, (src, dst) in enumerate(pairs)]
    for cp in copies:
        cp.start()
    for cp in copies:
        cp.wait()


def solution(mesh):
    def local(x_blk, b_own, c_full, ridge_lam):
        shapes = ((64, RANK), (RANK, 256), (32, RANK))
        operands = (x_blk, b_own.T, c_full)
        operands = [pltpu.with_memory_space_constraint(v, pltpu.HBM) for v in operands]
        dma = pltpu.SemaphoreType.DMA
        vm = pltpu.VMEM
        a_new, b_new, c_new = pl.pallas_call(
            kernel,
            out_shape=tuple(pltpu.VMEM(shape, F32) for shape in shapes),
            in_specs=[pl.BlockSpec(memory_space=pltpu.HBM)] * 3 + [pl.BlockSpec(memory_space=pltpu.SMEM)],
            out_specs=(pl.BlockSpec(memory_space=pltpu.VMEM),) * 3,
            scratch_shapes=[
                vm((RANK, J_TILE), F32),
                vm((2 * K_LOC, RANK), F32),
                vm((J_TILES, K_LOC, I_LOC, J_TILE), F32),
                vm((J_TILES, K_LOC, I_LOC, J_TILE), BF16),
                vm((J_TILES, K_LOC, J_TILE, I_LOC), BF16),
                vm((K_LOC, RANK, I_LOC), F32),
                vm((SWEEPS + 1, J_TILES, RANK, J_TILE), BF16),
                vm((RANK, LANES), F32),
                vm((RANK, LANES), F32),
                vm((K_LOC, RANK, LANES), F32),
                vm((A_CHUNKS, RANK, I_HALF), F32),
                vm((A_CHUNKS, RANK, I_HALF), BF16),
                vm((A_CHUNKS, RANK, I_HALF), F32),
                vm((SWEEPS, 3, A_CHUNKS, RANK, I_HALF), F32),
                vm((RANK, LANES), F32),
                vm((SWEEPS, RANK, LANES), F32),
                vm((J_TILES, RANK, J_TILE), F32),
                vm((SWEEPS, 2, RANK, J_TILE), F32),
                vm((2, RANK, J_TILE), F32),
                vm((SWEEPS, 2, RANK, J_TILE), F32),
                vm((2, RANK, J_TILE), F32),
                vm((RANK // 2, LANES), F32),
                vm((7, RANK // 2, LANES), F32),
                vm((RANK // 2, LANES), F32),
                vm((RANK // 2, LANES), F32),
                vm((SWEEPS, 3, RANK // 2, LANES), F32),
                vm((RANK, LANES), F32),
                vm((K_LOC // 2, LANES), F32),
                vm((SWEEPS, 7, K_LOC // 2, LANES), F32),
                vm((RANK, RANK), F32),
                dma((2,)), dma((J_TILES, K_LOC // LOAD_K)), dma((3,)), dma((3,)),
                dma((3, A_CHUNKS)), dma((SWEEPS, 3, A_CHUNKS)),
                dma, dma((SWEEPS,)),
                dma((2,)), dma((SWEEPS, 2)), dma((2,)), dma((SWEEPS, 2)),
                dma((2,)), dma((SWEEPS, 2)),
                dma((7,)), dma((7,)), dma((3,)), dma((SWEEPS, 3)),
                dma((7,)), dma((SWEEPS, 7)),
            ],
            compiler_params=pltpu.CompilerParams(collective_id=0, has_side_effects=True,
                                                 vmem_limit_bytes=52 * 1024 * 1024),
            name="als_sweeps",
        )(*operands, ridge_lam.reshape(1, 1))
        a_new, b_new, c_new = pl.pallas_call(
            emit,
            out_shape=tuple(jax.ShapeDtypeStruct(shape, F32) for shape in shapes),
            in_specs=[pl.BlockSpec(memory_space=pltpu.VMEM)] * 3,
            out_specs=(pl.BlockSpec(memory_space=pl.ANY),) * 3,
            scratch_shapes=[dma((3,))],
            compiler_params=pltpu.CompilerParams(vmem_limit_bytes=1024 * 1024),
            name="emit_factors",
        )(a_new, b_new, c_new)
        return a_new, b_new.T, c_new

    return jax.shard_map(
        local,
        mesh=mesh,
        in_specs=(P("tube", "row", "col"), P(("col", "row", "tube"), None), P(None, None), P()),
        out_specs=(P(("row", "col", "tube"), None), P(("col", "row", "tube"), None), P(None, None)),
        check_vma=False,
    )
```
